32 devices in a mesh: seq: 16 (over z, x, core), fsdp: 2 (over y).
Axes of the slice: x: 2, y: 2, z: 4, core: 2. Of those that a mesh axis runs over, the one named last changes fastest.
Arguments:
- hidden_next: bfloat16 [4096, 8192], P('seq'), may hold values from -6 to 6
- values_next: bfloat16 [4096, 8192], P('seq', 'fsdp'), may hold values from -6 to 6
- seg_next: int32 [4], replicated, may hold values from 1 to 2048, 4096 in all
- proj_bc: bfloat16 [8192, 1024], P(('seq', 'fsdp')), may hold values from -0.046875 to 0.046875
- proj_dt: bfloat16 [8192, 128], P(('seq', 'fsdp')), may hold values from -0.0625 to 0.0625
- dt_bias: float32 [128], replicated, may hold values from -4 to -2.5
- decay_rate: float32 [128], replicated, may hold values from 0 to 1, as said below
- skip_gain: float32 [128], replicated, may hold values from 0.5 to 1.5
- bc_prev: bfloat16 [4096, 1024], P('seq'), may hold values from -4 to 4
- dt_prev: float32 [4096, 128], P('seq', 'fsdp'), may hold values from 0.01 to 0.3
- seg_prev: int32 [4], replicated, may hold values from 1 to 2048, 4096 in all
- grad_prev: bfloat16 [4096, 8192], P('seq', 'fsdp'), may hold values from -6 to 6
Outputs:
- out_next: bfloat16 [4096, 8192], P('seq', 'fsdp')
- grad_values: bfloat16 [4096, 8192], P('seq', 'fsdp')
The draws below stay inside these ranges and needn't reach their ends.
Inputs may be any that keep to these rules, and one draw needn't show every extreme that they name: `seg_next`: lengths of the rollout's 4 segments in order, summing to 4096. `seg_prev`: lengths of the rollout's 4 segments in order, summing to 4096. `decay_rate`: positive.
All inputs are finite; a program needn't handle non-finite values.
Results may differ from the reference program's by a relative error of at most 0.0064.
Values may be sent and summed in bfloat16 or wider, within the bound.
A program may use at most 192 MiB of HBM per device.

```python
import math
import jax
import jax.numpy as jnp
import numpy as np
from jax import lax

D = 8192
HW = 128
P_SIZE = 64
GW = 4
N = 128
SPAN = 128
NSEG = 4
SEQ_LEN = 4096
BCW = 1024


def draw_decay_rate(key, part):
    streams = jax.random.split(jax.random.fold_in(key, 11), 3)
    lasting = jax.random.uniform(streams[0], (HW,)) < 0.5
    slow_rate = jnp.exp(jax.random.uniform(streams[1], (HW,), minval=jnp.log(5.0), maxval=jnp.log(20.0))) / SEQ_LEN
    fast_rate = jnp.exp(jax.random.uniform(streams[2], (HW,), minval=jnp.log(0.25), maxval=jnp.log(0.8)))
    return jnp.where(lasting, slow_rate, fast_rate).astype(jnp.float32)


def spiked(values, stream_key, source, target, blocks, factor):
    owner, partner = [(jnp.arange(values.shape[position]) // (values.shape[position] // blocks)).reshape([-1 if axis == position else 1 for axis in range(values.ndim)]) for position in (source, target)]
    chosen = jax.random.permutation(stream_key, blocks)[partner]
    strong = (owner == chosen) | (owner == (partner + blocks // 2) % blocks)
    return jnp.where(strong, factor * values, values)


def block_scale(rng, shape, cuts, least, largest):
    def one(axis_at, shards_of):
        heights = jax.random.uniform(jax.random.fold_in(jax.random.fold_in(rng, 6), axis_at), (shards_of,), jnp.float32, least / len(cuts), largest / len(cuts))
        return jnp.repeat(jnp.exp(heights), shape[axis_at] // shards_of).reshape((-1,) + (1,) * (len(shape) - axis_at - 1))

    factor_of = one(*cuts[0])
    for cut in cuts[1:]:
        factor_of = factor_of * one(*cut)
    return factor_of


def split_up(amount, total, reach, lean):
    loads = [(1 << 20) // math.isqrt(rank ** lean) + 1 for rank in range(2, amount + 1)]
    rest, counts = total - reach - (amount - 1), [1] * (amount - 1)
    while rest > 0:
        free = [i for i in range(amount - 1) if counts[i] < reach]
        pool, left = sum([loads[i] for i in free]), rest
        for i in free:
            extra = min(reach - counts[i], max(1, left * loads[i] // pool), rest)
            counts[i] = counts[i] + extra
            rest = rest - extra
    return np.array([reach] + counts)


def uneven(stream_key, count, total, limit, slope):
    if count == 2:
        one = jax.random.randint(stream_key, (), max(1, total - limit), min(limit, total - 1) + 1)
        return jnp.stack([one, total - one])
    sizes = jnp.asarray(split_up(count, total, limit, slope), jnp.int32)
    pairs = (count - 1) // 2
    donor, sink = sizes[1:1 + 2 * pairs:2], sizes[2:2 + 2 * pairs:2]
    slack = jnp.minimum(donor - 1, limit - sink)
    shifted = jax.random.randint(jax.random.fold_in(stream_key, 1), (pairs,), 0, 1 << 20) % (slack + 1)
    sizes = sizes.at[1:1 + 2 * pairs:2].set(donor - shifted).at[2:2 + 2 * pairs:2].set(sink + shifted)
    return sizes[jax.random.permutation(jax.random.fold_in(stream_key, 2), count)]


def noise(own_key, shape, scale, most, pieces=(), kind=jnp.bfloat16):
    factor_of = block_scale(own_key, shape, pieces, -0.22, 0.18) if pieces else 1.0
    drawn = jax.random.normal(own_key, shape, jnp.float32) * scale * factor_of
    return jnp.minimum(jnp.maximum(drawn, -most), most).astype(kind)


def bell_draw_with(stream_key, extent, width, most, cuts, heavy, held_as=jnp.bfloat16):
    entries = width * jax.random.normal(stream_key, extent, jnp.float32)
    if cuts:
        entries = entries * block_scale(stream_key, extent, cuts, -0.22, 0.18)
    return jnp.clip(spiked(entries, jax.random.fold_in(stream_key, 3), *heavy), -most, most).astype(held_as)


def setup_inputs(seed: int = 0) -> dict:
    splits = jax.random.split(jax.random.key(seed), 13)
    hidden_next = noise(splits[0], (SEQ_LEN, D), 1.0, 6.0, ((0, 16),))
    values_next = noise(splits[1], (SEQ_LEN, HW * P_SIZE), 1.0, 6.0, ((0, 16), (1, 2)))
    seg_next = uneven(splits[2], NSEG, SEQ_LEN, SEQ_LEN // 2, 2).astype(jnp.int32)
    proj_bc = bell_draw_with(splits[3], (D, BCW), (D * 8) ** -0.5, 0.046875, ((0, 32),), (0, 1, 32, 2.75))
    proj_dt = noise(splits[4], (D, HW), D ** -0.5, 0.0625, ((0, 32),))
    dt_bias = jnp.clip(jax.random.uniform(splits[5], (HW,), jnp.float32, -4.0, -2.5), -4.0, -2.5)
    decay_rate = draw_decay_rate(jax.random.fold_in(splits[12], 71), 0)
    skip_gain = jnp.clip(jax.random.uniform(splits[7], (HW,), jnp.float32, 0.5, 1.5), 0.5, 1.5)
    bc_prev = noise(splits[8], (SEQ_LEN, BCW), 0.3, 4.0, ((0, 16),))
    dt_prev = jnp.clip(jnp.exp(math.log(0.3) - 3.4011974 * jax.random.uniform(splits[9], (SEQ_LEN, HW), jnp.float32) ** block_scale(splits[9], (SEQ_LEN, HW), ((0, 16), (1, 2)), -0.2, 0.2)), 0.01, 0.3)
    seg_prev = uneven(splits[10], NSEG, SEQ_LEN, SEQ_LEN // 2, 2).astype(jnp.int32)
    grad_prev = noise(splits[11], (SEQ_LEN, HW * P_SIZE), 1.0, 6.0, ((0, 16), (1, 2)))
    return dict(hidden_next=hidden_next, values_next=values_next, seg_next=seg_next, proj_bc=proj_bc, proj_dt=proj_dt, dt_bias=dt_bias, decay_rate=decay_rate, skip_gain=skip_gain, bc_prev=bc_prev, dt_prev=dt_prev, seg_prev=seg_prev, grad_prev=grad_prev)


def segment_table(lengths, tokens_total):
    bounds = jnp.cumsum(lengths)[:-1].astype(jnp.int32)
    places = jnp.arange(tokens_total + 1, dtype=jnp.int32) - 1
    return jnp.sum((bounds[None, :] <= places[:, None]).astype(jnp.int32), axis=1)


def block_parts(bc_block, dt_block, seg_ext, decay_rate):
    span_len = bc_block.shape[0]
    half_cols = bc_block.shape[1] // 2
    b_vectors = bc_block[:, :half_cols].reshape(span_len, GW, N)
    c_vectors = bc_block[:, half_cols:].reshape(span_len, GW, N)
    before = seg_ext[0]
    segment = seg_ext[1:]
    cumulative = jnp.cumsum(-dt_block * decay_rate[None, :], axis=0)
    final_cum = cumulative[-1]
    places = jnp.arange(span_len)
    linked = (segment[:, None] == segment[None, :]) & (places[:, None] >= places[None, :])
    scores = jnp.einsum("tgn,sgn->gts", c_vectors.astype(jnp.float32), b_vectors.astype(jnp.float32),
                        precision=lax.Precision.HIGHEST)
    by_head = cumulative.T
    spread = by_head[:, :, None] - by_head[:, None, :]
    decays = jnp.exp(jnp.where(linked[None], spread, -jnp.inf))
    weighted = (decays * dt_block.T[:, None, :]).reshape(GW, HW // GW, span_len, span_len)
    mixing = (weighted * scores[:, None]).reshape(HW, span_len, span_len).astype(jnp.bfloat16)
    keep_final = (segment == segment[-1]).astype(jnp.float32)
    linked_in = (segment == before).astype(jnp.float32)
    send_factor = keep_final[:, None] * jnp.exp(final_cum[None, :] - cumulative) * dt_block
    read_factor = linked_in[:, None] * jnp.exp(cumulative)
    carry_decay = (segment[-1] == before).astype(jnp.float32) * jnp.exp(final_cum)
    return b_vectors, c_vectors, mixing, send_factor, read_factor, carry_decay


def outer_sum(values, vectors):
    span_len, heads_all, head_dim = values.shape
    grouped = values.reshape(span_len, GW, heads_all // GW, head_dim).astype(jnp.float32)
    result = jnp.einsum("sgqp,sgn->gqpn", grouped, vectors.astype(jnp.float32), precision=lax.Precision.HIGHEST)
    return result.reshape(heads_all, head_dim, vectors.shape[2])


def read_state(state_now, vectors, factor):
    heads_all, head_dim, state_dim = state_now.shape
    grouped = state_now.reshape(GW, heads_all // GW, head_dim, state_dim)
    result = jnp.einsum("gqpn,tgn->tgqp", grouped, vectors.astype(jnp.float32), precision=lax.Precision.HIGHEST)
    return result.reshape(vectors.shape[0], heads_all, head_dim) * factor[:, :, None]


def forward_rollout(hidden, inputs, lengths, proj_bc, proj_dt, dt_bias, decay_rate, skip_gain):
    dt_all = jax.nn.softplus(jnp.dot(hidden, proj_dt, preferred_element_type=jnp.float32) + dt_bias[None, :])
    bc_all = jnp.dot(hidden, proj_bc, preferred_element_type=jnp.float32).astype(jnp.bfloat16)
    seg_all = segment_table(lengths, SEQ_LEN)

    def advance(state_now, block_id):
        offset = (block_id * SPAN).astype(jnp.int32)
        bc_block = lax.dynamic_slice_in_dim(bc_all, offset, SPAN, 0)
        dt_block = lax.dynamic_slice_in_dim(dt_all, offset, SPAN, 0)
        seg_ext = lax.dynamic_slice_in_dim(seg_all, offset, SPAN + 1, 0)
        values = lax.dynamic_slice_in_dim(inputs, offset, SPAN, 0).reshape(SPAN, HW, P_SIZE)
        b_vectors, c_vectors, mixing, send_factor, read_factor, carry_decay = block_parts(
            bc_block, dt_block, seg_ext, decay_rate)
        inside = jnp.einsum("hts,shp->thp", mixing.astype(jnp.float32), values.astype(jnp.float32),
                            precision=lax.Precision.HIGHEST)
        output = inside + read_state(state_now, c_vectors, read_factor) + skip_gain[None, :, None] * values.astype(jnp.float32)
        scaled = (values.astype(jnp.float32) * send_factor[:, :, None]).astype(jnp.bfloat16)
        state_next = carry_decay[:, None, None] * state_now + outer_sum(scaled, b_vectors)
        return state_next, output.astype(jnp.bfloat16).reshape(SPAN, HW * P_SIZE)

    blocks_all = jnp.arange(SEQ_LEN // SPAN, dtype=jnp.int32)
    _, outputs = lax.scan(advance, jnp.zeros((HW, P_SIZE, N), jnp.float32), blocks_all)
    return outputs.reshape(SEQ_LEN, HW * P_SIZE)


def backward_rollout(bc_all, dt_all, lengths, grads_all, decay_rate, skip_gain):
    seg_all = segment_table(lengths, SEQ_LEN)

    def retreat(state_now, block_id):
        offset = (block_id * SPAN).astype(jnp.int32)
        bc_block = lax.dynamic_slice_in_dim(bc_all, offset, SPAN, 0)
        dt_block = lax.dynamic_slice_in_dim(dt_all, offset, SPAN, 0)
        seg_ext = lax.dynamic_slice_in_dim(seg_all, offset, SPAN + 1, 0)
        grad_block = lax.dynamic_slice_in_dim(grads_all, offset, SPAN, 0).reshape(SPAN, HW, P_SIZE)
        b_vectors, c_vectors, mixing, send_factor, read_factor, carry_decay = block_parts(
            bc_block, dt_block, seg_ext, decay_rate)
        inside = jnp.einsum("hts,thp->shp", mixing.astype(jnp.float32), grad_block.astype(jnp.float32),
                            precision=lax.Precision.HIGHEST)
        output = inside + read_state(state_now, b_vectors, send_factor) + skip_gain[None, :, None] * grad_block.astype(jnp.float32)
        scaled = (grad_block.astype(jnp.float32) * read_factor[:, :, None]).astype(jnp.bfloat16)
        state_next = carry_decay[:, None, None] * state_now + outer_sum(scaled, c_vectors)
        return state_next, output.astype(jnp.bfloat16).reshape(SPAN, HW * P_SIZE)

    blocks_all = jnp.arange(SEQ_LEN // SPAN, dtype=jnp.int32)
    _, outputs = lax.scan(retreat, jnp.zeros((HW, P_SIZE, N), jnp.float32), blocks_all, reverse=True)
    return outputs.reshape(SEQ_LEN, HW * P_SIZE)


def reference(hidden_next, values_next, seg_next, proj_bc, proj_dt, dt_bias, decay_rate, skip_gain,
              bc_prev, dt_prev, seg_prev, grad_prev):
    out_next = forward_rollout(hidden_next, values_next, seg_next, proj_bc, proj_dt, dt_bias, decay_rate, skip_gain)
    grad_values = backward_rollout(bc_prev, dt_prev, seg_prev, grad_prev, decay_rate, skip_gain)
    return out_next, grad_values
```

```python
import functools

import jax
import jax.numpy as jnp
from jax import lax
from jax.experimental import pallas as pl
from jax.experimental.pallas import tpu as pltpu
from jax.sharding import PartitionSpec as P

GW = 4
SPAN = 128
LANES = 128
MESH = pl.DeviceIdType.MESH


def widen(a, c, head_dim):
    per = LANES // head_dim
    lane = lax.broadcasted_iota(jnp.int32, (1, LANES), 1)
    res = a[:, c * per:c * per + 1]
    for k in range(1, per):
        res = jnp.where(lane >= k * head_dim, a[:, c * per + k:c * per + k + 1], res)
    return jnp.broadcast_to(res, (a.shape[0], LANES))


def seg_maker(len_ref):
    bound = []
    total = jnp.int32(0)
    for k in range(len_ref.shape[0] - 1):
        total = total + len_ref[k]
        bound.append(total)

    def seg_of(pos):
        s = jnp.zeros_like(pos)
        for b in bound:
            s = s + (b <= pos).astype(jnp.int32)
        return s

    return seg_of


def local_states(back, dims, len_ref, x_ref, q_ref, dt_ref, decay_ref, work, pre, keep):
    nblocks, heads, groups, head_dim = dims
    cum_s, cum_t, dt_t, fout_s = work
    npair = heads * head_dim // LANES
    pair_group = npair // groups
    seg_of = seg_maker(len_ref)
    slab = lax.axis_index("seq") * (nblocks * SPAN)
    dim0 = lax.broadcasted_iota(jnp.int32, (SPAN, SPAN), 0)
    dim1 = lax.broadcasted_iota(jnp.int32, (SPAN, SPAN), 1)
    tril = (dim0 >= dim1).astype(jnp.float32)
    for c in range(npair):
        pre[0, c] = jnp.zeros((LANES, LANES), jnp.float32)
        keep[0, c] = jnp.ones((1, LANES), jnp.float32)
    for step in range(nblocks):
        b = nblocks - 1 - step if back else step
        rows = slice(b * SPAN, (b + 1) * SPAN)
        dt = dt_ref[rows, :]
        cum = jnp.dot(tril, -(dt * decay_ref[...]), precision=lax.Precision.HIGHEST,
                      preferred_element_type=jnp.float32)
        end = cum[SPAN - 1:SPAN, :]
        cum_s[rows, :] = cum
        cum_t[b] = cum.T
        dt_t[b] = dt.T
        seg = seg_of(slab + b * SPAN + lax.broadcasted_iota(jnp.int32, (SPAN, heads), 0))
        edge = slab + b * SPAN + lax.broadcasted_iota(jnp.int32, (1, heads), 0) * 0
        seg_e = seg_of(edge + (SPAN - 1))
        seg_b = jnp.where(edge == 0, 0, seg_of(edge - 1))
        send = jnp.where(seg == seg_e, jnp.exp(end - cum), 0.0) * dt
        read = jnp.where(seg == seg_b, jnp.exp(cum), 0.0)
        carry = jnp.where(seg_e == seg_b, jnp.exp(end), 0.0)
        f_in = read if back else send
        fout_s[rows, :] = send if back else read
        qt = [q_ref[rows, g * LANES:(g + 1) * LANES].T for g in range(groups)]
        for c in range(npair):
            cols = slice(c * LANES, (c + 1) * LANES)
            sent = (x_ref[rows, cols].astype(jnp.float32) * widen(f_in, c, head_dim)).astype(jnp.bfloat16)
            loc = jnp.dot(qt[c // pair_group], sent, preferred_element_type=jnp.float32)
            wide = widen(carry, c, head_dim)
            pre[step + 1, c] = wide * pre[step, c] + loc
            keep[step + 1, c] = wide * keep[step, c]


def in_block(back, dims, len_ref, x_ref, p_ref, q_ref, dt_ref, skip_ref, work, inside, fexp, span=None):
    nblocks, heads, groups, head_dim = dims
    cum_s, cum_t, dt_t, fout_s = work
    npair = heads * head_dim // LANES
    per = LANES // head_dim
    pair_group = npair // groups
    seg_of = seg_maker(len_ref)
    slab = lax.axis_index("seq") * (nblocks * SPAN)
    dim0 = lax.broadcasted_iota(jnp.int32, (SPAN, SPAN), 0)
    dim1 = lax.broadcasted_iota(jnp.int32, (SPAN, SPAN), 1)
    lane = lax.broadcasted_iota(jnp.int32, (1, LANES), 1)

    def one(b, _):
        start = pl.multiple_of(b * SPAN, SPAN)
        rows = pl.ds(start, SPAN)
        seg_i = seg_of(slab + start + dim0)
        seg_j = seg_of(slab + start + dim1)
        order = (dim1 >= dim0) if back else (dim1 <= dim0)
        bias = jnp.where((seg_i == seg_j) & order, 0.0, -jnp.inf)
        cum = cum_s[rows, :]
        dt = dt_ref[rows, :]
        f_out = fout_s[rows, :]
        for g in range(groups):
            gl = slice(g * LANES, (g + 1) * LANES)
            score = lax.dot_general(p_ref[rows, gl], q_ref[rows, gl], (((1,), (1,)), ((), ())),
                                    preferred_element_type=jnp.float32)
            for c in range(g * pair_group, (g + 1) * pair_group):
                cols = slice(c * LANES, (c + 1) * LANES)
                x = x_ref[rows, cols]
                mixes, parts = [], []
                for k in range(per):
                    h = c * per + k
                    col = cum[:, h:h + 1]
                    row = cum_t[b, h:h + 1, :]
                    spread = (row - col) if back else (col - row)
                    w = jnp.exp(spread + bias) * score
                    if not back:
                        w = w * dt_t[b, h:h + 1, :]
                    mixes.append(w.astype(jnp.bfloat16))
                    mine = (lane >= k * head_dim) & (lane < (k + 1) * head_dim)
                    parts.append(jnp.where(mine, x, jnp.zeros_like(x)))
                acc = jnp.dot(jnp.concatenate(mixes, 1), jnp.concatenate(parts, 0),
                              preferred_element_type=jnp.float32)
                if back:
                    acc = acc * widen(dt, c, head_dim)
                inside[c, rows, :] = acc + widen(skip_ref[...], c, head_dim) * x.astype(jnp.float32)
                fexp[c, rows, :] = widen(f_out, c, head_dim)
        return 0

    first, last = (0, nblocks) if span is None else span
    lax.fori_loop(first, last, one, 0)


HOP_CHUNKS = 5


def chain_kernel(count, dims, len_ref, x_ref, p_ref, q_ref, dt_ref, decay_ref, skip_ref,
                 lenb_ref, xb_ref, pb_ref, qb_ref, dtb_ref,
                 out_ref, grad_ref, *scratch):
    work, work_b, rest = scratch[:4], scratch[4:8], scratch[12:]
    inside_b, fexp_b, pre_b, keep_b = scratch[8:12]
    inside, fexp, pre, keep, inbox, outbox, in_b, out_b, s_sem, r_sem, sb_sem, rb_sem = rest
    nblocks, heads, groups, head_dim = dims
    npair = heads * head_dim // LANES
    pair_group = npair // groups
    me = lax.axis_index("seq")
    low, high = me == 0, me == count - 1

    barrier = pltpu.get_barrier_semaphore()

    @pl.when(jnp.logical_not(low))
    def _():
        pl.semaphore_signal(barrier, inc=1, device_id={"seq": me - 1}, device_id_type=MESH)

    @pl.when(jnp.logical_not(high))
    def _():
        pl.semaphore_signal(barrier, inc=1, device_id={"seq": me + 1}, device_id_type=MESH)

    local_states(False, dims, len_ref, x_ref, q_ref, dt_ref, decay_ref, work, pre, keep)
    local_states(True, dims, lenb_ref, xb_ref, qb_ref, dtb_ref, decay_ref, work_b, pre_b, keep_b)

    @pl.when(low)
    def _():
        inbox[...] = jnp.zeros_like(inbox)

    @pl.when(high)
    def _():
        in_b[...] = jnp.zeros_like(in_b)

    pl.semaphore_wait(barrier, jnp.where(low, 0, 1) + jnp.where(high, 0, 1))

    def hop(back, c):
        return pltpu.make_async_remote_copy(
            src_ref=(out_b if back else outbox).at[c], dst_ref=(in_b if back else inbox).at[c],
            send_sem=(sb_sem if back else s_sem).at[c], recv_sem=(rb_sem if back else r_sem).at[c],
            device_id={"seq": me - 1 if back else me + 1}, device_id_type=MESH)

    def relay(back, c):
        first, last = (high, low) if back else (low, high)
        kp, pr = (keep_b, pre_b) if back else (keep, pre)

        @pl.when(jnp.logical_not(first))
        def _():
            hop(back, c).wait_recv()

        @pl.when(jnp.logical_not(last))
        def _():
            state = (in_b if back else inbox)[c].astype(jnp.float32)
            (out_b if back else outbox)[c] = (kp[nblocks, c] * state + pr[nblocks, c]).astype(jnp.bfloat16)
            hop(back, c).start()

    def finish(back, c):
        kp, pr, ins, fx, vec, out = (
            (keep_b, pre_b, inside_b, fexp_b, pb_ref, grad_ref) if back
            else (keep, pre, inside, fexp, p_ref, out_ref))
        g = c // pair_group
        cols = pl.ds(pl.multiple_of(c * LANES, LANES), LANES)
        gl = pl.ds(pl.multiple_of(g * LANES, LANES), LANES)
        state = (in_b if back else inbox)[c].astype(jnp.float32)
        for step in range(nblocks):
            b = nblocks - 1 - step if back else step
            rows = slice(b * SPAN, (b + 1) * SPAN)
            entering = (kp[step, c] * state + pr[step, c]).astype(jnp.bfloat16)
            y = jnp.dot(vec[rows, gl], entering, preferred_element_type=jnp.float32)
            out[rows, cols] = (ins[c, rows, :] + fx[c, rows, :] * y).astype(jnp.bfloat16)

    lag = (2 * me - (count - 1)) * HOP_CHUNKS
    up_first = lag < 0
    gap = jnp.where(up_first, -lag, lag)
    block_at = jnp.where(gap >= npair, npair, 0)

    def step_of(i, _):
        @pl.when(i == block_at)
        def _():
            in_block(False, dims, len_ref, x_ref, p_ref, q_ref, dt_ref, skip_ref, work, inside, fexp)
            in_block(True, dims, lenb_ref, xb_ref, pb_ref, qb_ref, dtb_ref, skip_ref, work_b, inside_b, fexp_b)

        for back in (False, True):
            leads = jnp.logical_not(up_first) if back else up_first
            c = i - jnp.where(leads, 0, gap)

            @pl.when((c >= 0) & (c < npair))
            def _(back=back, c=c):
                relay(back, c)

            done = jnp.where(leads, i - npair, c)

            @pl.when((done >= 0) & (done < npair))
            def _(back=back, done=done):
                finish(back, done)

        return 0

    lax.fori_loop(0, npair + jnp.maximum(gap, npair), step_of, 0)

    def drain(c, _):
        @pl.when(jnp.logical_not(high))
        def _():
            hop(False, c).wait_send()

        @pl.when(jnp.logical_not(low))
        def _():
            hop(True, c).wait_send()

        return 0

    lax.fori_loop(0, npair, drain, 0)


def sizes_of(x, p_vec, dt):
    tokens, width = x.shape
    heads = dt.shape[1]
    dims = (tokens // SPAN, heads, p_vec.shape[1] // LANES, width // heads)
    nblocks, npair = dims[0], width // LANES
    f32 = jnp.float32
    work = [pltpu.VMEM((tokens, heads), f32), pltpu.VMEM((nblocks, heads, SPAN), f32),
            pltpu.VMEM((nblocks, heads, SPAN), f32), pltpu.VMEM((tokens, heads), f32)]
    kept = [(npair, tokens, LANES), (npair, tokens, LANES),
            (nblocks + 1, npair, LANES, LANES), (nblocks + 1, npair, 1, LANES)]
    return dims, npair, work, kept


VM = pl.BlockSpec(memory_space=pltpu.VMEM)
SM = pl.BlockSpec(memory_space=pltpu.SMEM)


def chains(lengths, x, p_vec, q_vec, dt, decay, skip, *back):
    dims, npair, work, kept = sizes_of(x, p_vec, dt)
    box = pltpu.VMEM((npair, LANES, LANES), jnp.bfloat16)
    sem = pltpu.SemaphoreType.DMA((npair,))
    return pl.pallas_call(
        functools.partial(chain_kernel, lax.axis_size("seq"), dims),
        out_shape=[jax.ShapeDtypeStruct(x.shape, jnp.bfloat16)] * 2,
        in_specs=[SM] + [VM] * 6 + [SM] + [VM] * 4,
        out_specs=[VM] * 2,
        scratch_shapes=(work * 2 + [pltpu.VMEM(k, jnp.float32) for k in kept] * 2
                        + [box] * 4 + [sem] * 4),
        compiler_params=pltpu.CompilerParams(
            collective_id=0, has_side_effects=True, vmem_limit_bytes=56 * 1024 * 1024),
        cost_estimate=pl.CostEstimate(flops=40_000_000_000, bytes_accessed=40_000_000, transcendentals=0),
        name="chains",
    )(lengths, x, p_vec, q_vec, dt, decay, skip, *back)


PIECES = 4


def gather_kernel(count, h_ref, w_ref, bc_ref, dt_ref,
                  held, acc, bc_out, bc_in, dt_out, dt_in,
                  ring_s, ring_r, side_s, side_r, x_s, x_r):
    me, f = lax.axis_index("seq"), lax.axis_index("fsdp")
    n = count // 2
    half_ring = n // 2
    core, chip = me % 2, me // 2
    r = jnp.where(chip % 2 == 0, chip // 2, n - 1 - chip // 2)
    rows = w_ref.shape[0]
    piece = rows // PIECES
    wide = bc_ref.shape[1]

    def id_of(pos, which):
        p = (pos + 2 * n) % n
        up = p < half_ring
        return jnp.where(up, p * 2, (n - 1 - p) * 2 + 1) * 2 + which

    nxt, prv, partner = id_of(r + 1, core), id_of(r - 1, core), chip * 2 + 1 - core

    barrier = pltpu.get_barrier_semaphore()
    for peer in (nxt, prv, partner):
        pl.semaphore_signal(barrier, inc=1, device_id={"seq": peer}, device_id_type=MESH)
    pl.semaphore_signal(barrier, inc=1, device_id={"fsdp": 1 - f}, device_id_type=MESH)
    pl.semaphore_wait(barrier, 4)

    def part(p):
        return pl.ds(p * piece, piece)

    def origin(step, p, which):
        return id_of(r - step if p < PIECES // 2 else r + step, which)

    def ring_copy(step, p, src):
        return pltpu.make_async_remote_copy(
            src_ref=src, dst_ref=held.at[origin(step, p, core), part(p), :],
            send_sem=ring_s.at[step, p], recv_sem=ring_r.at[step, p],
            device_id={"seq": nxt if p < PIECES // 2 else prv}, device_id_type=MESH)

    def side_copy(step, p, src):
        return pltpu.make_async_remote_copy(
            src_ref=src, dst_ref=held.at[origin(step, p, core), part(p), :],
            send_sem=side_s.at[step, p], recv_sem=side_r.at[step, p],
            device_id={"seq": partner}, device_id_type=MESH)

    def landed(step, p):
        return held.at[origin(step, p, core), part(p), :]

    for p in range(PIECES):
        ring_copy(0, p, w_ref.at[part(p), :]).start()
    for p in range(PIECES):
        side_copy(0, p, w_ref.at[part(p), :]).start()

    def columns(seq_index, first):
        start = (seq_index * 2 + f) * rows + first
        return h_ref[:, pl.ds(pl.multiple_of(start, rows // 2), rows // 2)]

    def mac(step, which):
        half = rows // 2
        lo, hi = origin(step, 0, which), origin(step, PIECES - 1, which)
        left = jnp.concatenate([columns(lo, 0), columns(hi, half)], axis=1)
        right = jnp.concatenate([held[lo, 0:half, :], held[hi, half:, :]], axis=0)
        acc[...] += jnp.dot(left, right, preferred_element_type=jnp.float32)

    acc[...] = jnp.dot(jnp.concatenate([columns(me, 0), columns(me, rows // 2)], axis=1), w_ref[...],
                       preferred_element_type=jnp.float32)

    def one(step, _):
        for p in (0, PIECES // 2, 1, PIECES // 2 + 1):
            ring_copy(step, p, landed(step, p)).wait_recv()

            @pl.when(step < n - 2)
            def _(p=p):
                ring_copy(step + 1, p, landed(step + 1, p)).start()

            side_copy(step + 1, p, landed(step + 1, p)).start()
        mac(step + 1, core)
        for p in range(PIECES):
            side_copy(step, p, landed(step, p)).wait_recv()
        mac(step, 1 - core)
        return 0

    lax.fori_loop(0, n - 1, one, 0)
    for p in range(PIECES):
        side_copy(n - 1, p, landed(n - 1, p)).wait_recv()
    mac(n - 1, 1 - core)

    def cross(src, dst, k):
        return pltpu.make_async_remote_copy(
            src_ref=src, dst_ref=dst, send_sem=x_s.at[k], recv_sem=x_r.at[k],
            device_id={"fsdp": 1 - f}, device_id_type=MESH)

    def side_of(which):
        return pl.ds(pl.multiple_of(which * wide, wide), wide)

    bc_out[...] = acc[:, side_of(1 - f)]
    dt_out[...] = acc[:, 2 * wide:]
    cross(bc_out, bc_in, 0).start()
    cross(dt_out, dt_in, 1).start()

    def drain(step, _):
        for p in range(PIECES):
            @pl.when(step < n - 1)
            def _(p=p):
                ring_copy(step, p, landed(step, p)).wait_send()

            side_copy(step, p, landed(step, p)).wait_send()
        return 0

    lax.fori_loop(0, n, drain, 0)
    cross(bc_out, bc_in, 0).wait()
    bc_ref[...] = (acc[:, side_of(f)] + bc_in[...]).astype(jnp.bfloat16)
    cross(dt_out, dt_in, 1).wait()
    dt_ref[...] = acc[:, 2 * wide:] + dt_in[...]


def gathered_sums(hidden, shard, wide):
    count = lax.axis_size("seq")
    tokens, total = hidden.shape[0], shard.shape[1]
    f32, bf16 = jnp.float32, jnp.bfloat16
    n = count // 2
    dma = pltpu.SemaphoreType.DMA
    return pl.pallas_call(
        functools.partial(gather_kernel, count),
        out_shape=[jax.ShapeDtypeStruct((tokens, wide), bf16),
                   jax.ShapeDtypeStruct((tokens, total - 2 * wide), f32)],
        in_specs=[VM] * 2,
        out_specs=[VM] * 2,
        scratch_shapes=[
            pltpu.VMEM((count,) + shard.shape, bf16),
            pltpu.VMEM((tokens, total), f32),
            pltpu.VMEM((tokens, wide), f32), pltpu.VMEM((tokens, wide), f32),
            pltpu.VMEM((tokens, total - 2 * wide), f32), pltpu.VMEM((tokens, total - 2 * wide), f32),
            dma((n, PIECES)), dma((n, PIECES)), dma((n, PIECES)), dma((n, PIECES)), dma((2,)), dma((2,)),
        ],
        compiler_params=pltpu.CompilerParams(
            collective_id=1, has_side_effects=True, vmem_limit_bytes=32 * 1024 * 1024),
        cost_estimate=pl.CostEstimate(flops=40_000_000_000, bytes_accessed=40_000_000, transcendentals=0),
        name="gather_project",
    )(hidden, shard)


Z_LAG = 4
CORE_LAG = 3


def fused_kernel(count, dims, len_ref, lenb_ref, bias_in, decay_in, skip_in, pdt_ref, dtt_ref,
                 h_hbm, x_hbm, w_hbm, bcp_hbm, g_hbm, out_hbm, grad_hbm,
                 hid, held, yout, xv, gv, bp, cp, bn, cn, acc, dtn, dtp, decay_ref, skip_ref,
                 *scratch):
    work, work_b = scratch[:4], scratch[4:8]
    kept = (scratch[8:12], scratch[12:16])
    lout, lin, xout, xin, zout, zin, eout, ein, kv, ksib, kxo, kxi = (
        (scratch[16 + 2 * i], scratch[17 + 2 * i]) for i in range(12))
    (ld, ring_s, ring_r, side_s, side_r, y_s, y_r, l_s, l_r, k_s, k_r, c_s, c_r, z_s, z_r,
     e_s, e_r, o_sem) = scratch[40:]
    nblocks, heads, groups, head_dim = dims
    npair = heads * head_dim // LANES
    pair_group = npair // groups
    half_pairs = npair // 2
    me, f = lax.axis_index("seq"), lax.axis_index("fsdp")
    core, chip = me % 2, me // 2
    xpos, zpos, nz = chip % 2, chip // 2, count // 4
    n = count // 2
    half_ring = n // 2
    full = half_ring - 1
    far = 2 * full + 1
    gw = groups * LANES
    wrows = w_hbm.shape[0]
    prow = held.shape[2] // 2
    r = jnp.where(xpos == 0, zpos, n - 1 - zpos)

    def chip_at(pos):
        p = (pos + 2 * n) % n
        return jnp.where(p < half_ring, p * 2, (n - 1 - p) * 2 + 1)

    nxt, prv = chip_at(r + 1) * 2 + core, chip_at(r - 1) * 2 + core
    partner = chip * 2 + 1 - core
    xpeer = (zpos * 2 + 1 - xpos) * 2 + core
    own, other = core * 2 + f, core * 2 + 1 - f

    def at_cols(start):
        return pl.ds(pl.multiple_of(start, LANES), gw)

    def load(src, dst, k):
        return pltpu.make_async_copy(src, dst, ld.at[k])

    w_half = w_hbm.shape[1] // 2
    w_loads = [
        load(w_hbm.at[:, at_cols(f * gw)], held.at[chip, own, 0:wrows, 0:gw], 0),
        load(w_hbm.at[:, at_cols(w_half + f * gw)], held.at[chip, own, 0:wrows, gw:2 * gw], 1),
        load(w_hbm.at[:, at_cols((1 - f) * gw)], yout.at[0:wrows, 0:gw], 2),
        load(w_hbm.at[:, at_cols(w_half + (1 - f) * gw)], yout.at[0:wrows, gw:2 * gw], 3),
    ]
    b_loads = [
        load(g_hbm, gv, 4),
        load(bcp_hbm.at[:, at_cols(f * gw)], bp, 5),
        load(bcp_hbm.at[:, at_cols(w_half + f * gw)], cp, 6),
    ]
    h_load, x_load = load(h_hbm, hid, 7), load(x_hbm, xv, 8)
    for copy in (*w_loads, *b_loads, h_load, x_load):
        copy.start()

    barrier = pltpu.get_barrier_semaphore()
    for peer in (partner, xpeer):
        pl.semaphore_signal(barrier, inc=1, device_id={"seq": peer}, device_id_type=MESH)
    pl.semaphore_signal(barrier, inc=1, device_id={"fsdp": 1 - f}, device_id_type=MESH)

    @pl.when(zpos > 0)
    def _():
        pl.semaphore_signal(barrier, inc=1, device_id={"seq": me - 4}, device_id_type=MESH)

    @pl.when(zpos < nz - 1)
    def _():
        pl.semaphore_signal(barrier, inc=1, device_id={"seq": me + 4}, device_id_type=MESH)

    lane = lax.broadcasted_iota(jnp.int32, (LANES, LANES), 1)
    top = pdt_ref[0:LANES, :].astype(jnp.float32)
    low = pdt_ref[LANES:2 * LANES, :].astype(jnp.float32)
    pack0 = jnp.where(lane < heads, top, pltpu.roll(low, heads, 1))
    pack1 = jnp.where(lane < heads, pltpu.roll(top, heads, 1), low)
    mine = jnp.where(f == 0, pack0, pack1).astype(jnp.bfloat16)
    theirs = jnp.where(f == 0, pack1, pack0).astype(jnp.bfloat16)
    strips = 2 * gw // LANES
    strip = LANES // strips
    for k in range(strips):
        lanes = slice(k * LANES, (k + 1) * LANES)
        held[chip, own, wrows:wrows + strip, lanes] = mine[k * strip:(k + 1) * strip, :]
        yout[wrows:wrows + strip, lanes] = theirs[k * strip:(k + 1) * strip, :]
    decay_ref[...] = jnp.where(f == 0, decay_in[:, 0:heads], decay_in[:, heads:2 * heads])
    skip_ref[...] = jnp.where(f == 0, skip_in[:, 0:heads], skip_in[:, heads:2 * heads])
    bias = jnp.where(f == 0, bias_in[:, 0:heads], bias_in[:, heads:2 * heads])
    for b in range(nblocks):
        dtp[b * SPAN:(b + 1) * SPAN, :] = dtt_ref[:, b * SPAN:(b + 1) * SPAN].T

    pl.semaphore_wait(barrier, 3 + jnp.where(zpos > 0, 1, 0) + jnp.where(zpos < nz - 1, 1, 0))
    for copy in w_loads:
        copy.wait()

    def rows_of(j):
        return pl.ds((j % 2) * prow, prow)

    def piece(where, j, mine=True):
        base = (core if mine else 1 - core) * 2
        return held.at[where, base + (f if j < 2 else 1 - f), rows_of(j), :]

    def remote(src, dst, s, rv, **peer):
        return pltpu.make_async_remote_copy(src_ref=src, dst_ref=dst, send_sem=s, recv_sem=rv,
                                            device_id=peer, device_id_type=MESH)

    def ring(d, k, j, arrived=False):
        away = k if arrived else k - 1
        ref = piece(chip_at(r - away if d == 0 else r + away), j)
        return remote(ref, ref, ring_s.at[d, k - 1, j], ring_r.at[d, k - 1, j],
                      seq=nxt if d == 0 else prv)

    def chip_of(u):
        return chip_at(r - u if u <= full else (r + (u - full) if u < far else r + half_ring))

    def side(u, j, arrived=False):
        ref = piece(chip_of(u), j, not arrived)
        return remote(ref, ref, side_s.at[u, j], side_r.at[u, j], seq=partner)

    def cross(j, arrived=False):
        dst = held.at[chip, other, rows_of(j), :]
        dst = dst if arrived else held.at[chip, own, rows_of(j), :]
        return remote(yout.at[rows_of(j), :], dst, y_s.at[j], y_r.at[j], fsdp=1 - f)

    def begin(j):
        ring(0, 1, j).start()
        ring(1, 1, j).start()
        side(0, j).start()

    for j in range(2):
        cross(j).start()
        begin(j)

    def receive(k, j):
        for d in range(2):
            if k > full and (j < 2) != (d == 0):
                continue
            ring(d, k, j, True).wait_recv()
            if k < full or (k == full and (j < 2) == (d == 0)):
                ring(d, k + 1, j).start()
            side(far if k > full else (k if d == 0 else full + k), j).start()

    def mac(u, first=False):
        for j in range(4):
            side(u, j, True).wait_recv()
        q = chip_of(u)
        wide = 4 * wrows
        left = hid[:, pl.ds(pl.multiple_of(q * wide, wide), wide)]
        main = jnp.dot(left, jnp.concatenate([held[q, s, 0:wrows, :] for s in range(4)], axis=0),
                       preferred_element_type=jnp.float32)
        packs = jnp.concatenate(
            [held[q, s, wrows:wrows + strip, k * LANES:(k + 1) * LANES]
             for s in range(4) for k in range(strips)], axis=0)
        parts = [jnp.dot(jnp.concatenate([left[:, s * wrows + o:s * wrows + o + LANES] for s in range(4)], axis=1),
                         packs, preferred_element_type=jnp.float32) for o in (0, LANES)]
        for at, value in ((0, main), (2 * gw, parts[0]), (2 * gw + LANES, parts[1])):
            cols = slice(at, at + value.shape[1])
            acc[:, cols] = value if first else acc[:, cols] + value

    def my_half(back):
        return core * half_pairs

    def exchange(back):
        pre, keep = kept[back][2:]
        for c in range(npair):
            kv[back][c:c + 1, :] = keep[nblocks, c]
        remote(kv[back], ksib[back], k_s.at[back], k_r.at[back], seq=partner).start()

        def put(i, _):
            lout[back][i] = pre[nblocks, (1 - core) * half_pairs + i].astype(jnp.bfloat16)
            remote(lout[back].at[i], lin[back].at[i], l_s.at[back, i], l_r.at[back, i], seq=partner).start()
            return 0

        lax.fori_loop(0, half_pairs, put, 0)

    def lead_core(back):
        return (core == 1) if back else (core == 0)

    def lead_x(back):
        return (xpos == 1) if back else (xpos == 0)

    def row(ref, i):
        return ref[pl.ds(i, 1), :]

    def x_copy(back, i):
        return remote(xout[back].at[i], xin[back].at[i], c_s.at[back, i], c_r.at[back, i], seq=xpeer)

    def kx_copy(back):
        return remote(kxo[back], kxi[back], k_s.at[2 + back], k_r.at[2 + back], seq=xpeer)

    def combine(back):
        pre = kept[back][2]
        rows = pl.ds(pl.multiple_of(core * half_pairs, half_pairs), half_pairs)
        remote(kv[back], ksib[back], k_s.at[back], k_r.at[back], seq=partner).wait_recv()
        kxo[back][...] = kv[back][rows, :] * ksib[back][rows, :]
        kx_copy(back).start()

        def put(i, _):
            g = core * half_pairs + i
            remote(lout[back].at[i], lin[back].at[i], l_s.at[back, i], l_r.at[back, i], seq=partner).wait_recv()
            lead = lead_core(back)
            total = (pre[nblocks, g] * jnp.where(lead, row(ksib[back], g), 1.0)
                     + lin[back][i].astype(jnp.float32) * jnp.where(lead, 1.0, row(kv[back], g)))
            xout[back][i] = total.astype(jnp.bfloat16)
            x_copy(back, i).start()
            return 0

        lax.fori_loop(0, half_pairs, put, 0)

    def z_copy(back, i):
        return remote(zout[back].at[i], zin[back].at[i], z_s.at[back, i], z_r.at[back, i],
                      seq=me - 4 if back else me + 4)

    def e_copy(back, i):
        return remote(eout[back].at[i], ein[back].at[i], e_s.at[back, i], e_r.at[back, i], seq=partner)

    def out_copy(back, c):
        cols = pl.ds(pl.multiple_of(c * LANES, LANES), LANES)
        src, dst = (gv, grad_hbm) if back else (xv, out_hbm)
        return pltpu.make_async_copy(src.at[:, cols], dst.at[:, cols], o_sem.at[back, c])

    def finish(back, c, state):
        ins, fx, pre, keep = kept[back]
        vec, out = (bp, gv) if back else (cn, xv)
        cols = pl.ds(pl.multiple_of(c * LANES, LANES), LANES)
        gl = pl.ds(pl.multiple_of((c // pair_group) * LANES, LANES), LANES)
        for step in range(nblocks):
            b = nblocks - 1 - step if back else step
            rows = slice(b * SPAN, (b + 1) * SPAN)
            entering = state if step == 0 else keep[step, c] * state + pre[step, c]
            y = jnp.dot(vec[rows, gl], entering.astype(jnp.bfloat16), preferred_element_type=jnp.float32)
            out[rows, cols] = (ins[c, rows, :] + fx[c, rows, :] * y).astype(jnp.bfloat16)
        out_copy(back, c).start()

    def relay(back, i):
        pre = kept[back][2]
        g = core * half_pairs + i
        z_first, z_last = (zpos == nz - 1, zpos == 0) if back else (zpos == 0, zpos == nz - 1)
        x_copy(back, i).wait_recv()

        @pl.when(jnp.logical_not(z_first))
        def _():
            z_copy(back, i).wait_recv()

        k_own, k_peer = row(kxo[back], i), row(kxi[back], i)
        l_own, l_peer = xout[back][i].astype(jnp.float32), xin[back][i].astype(jnp.float32)
        state = jnp.where(z_first, 0.0, zin[back][i].astype(jnp.float32))
        lead = lead_x(back)
        zout[back][i] = (k_own * k_peer * state + l_own * jnp.where(lead, k_peer, 1.0)
                         + l_peer * jnp.where(lead, 1.0, k_own)).astype(jnp.bfloat16)

        @pl.when(jnp.logical_not(z_last))
        def _():
            z_copy(back, i).start()

        state = jnp.where(lead, state, k_peer * state + l_peer)
        head = lead_core(back)
        k_lead = jnp.where(head, row(kv[back], g), row(ksib[back], g))
        l_lead = jnp.where(head, pre[nblocks, g], lin[back][i].astype(jnp.float32))
        after = k_lead * state + l_lead
        eout[back][i] = jnp.where(head, after, state).astype(jnp.bfloat16)
        e_copy(back, i).start()
        finish(back, g, jnp.where(head, state, after))

    def settle(back, i):
        e_copy(back, i).wait_recv()
        finish(back, (1 - core) * half_pairs + i, ein[back][i].astype(jnp.float32))

    for copy in b_loads:
        copy.wait()
    local_states(True, dims, lenb_ref, gv, cp, dtp, decay_ref, work_b, *kept[1][2:])
    for j in range(2):
        cross(j, True).wait_recv()
        begin(j + 2)
    exchange(1)
    receive(1, 0)
    receive(1, 1)

    def block(back, b):
        if back:
            in_block(True, dims, lenb_ref, gv, bp, cp, dtp, skip_ref, work_b, *kept[1][:2], span=(b, b + 1))
        else:
            in_block(False, dims, len_ref, xv, cn, bn, dtn, skip_ref, work, *kept[0][:2])

    block(True, 0)
    receive(1, 2)
    receive(1, 3)
    block(True, 1)
    h_load.wait()
    for k in range(2, full + 1):
        for j in range(4):
            receive(k, j)
            if j == 1 and k == full:
                combine(1)
        if k == 2:
            mac(0, True)
        for u in (k - 1, full + k - 1):
            mac(u)
    for u in (full, 2 * full):
        mac(u)
    for j in range(4):
        receive(full + 1, j)
    mac(far)

    bn[...] = acc[:, 0:gw].astype(jnp.bfloat16)
    cn[...] = acc[:, gw:2 * gw].astype(jnp.bfloat16)
    at = 2 * gw
    dt_sum = acc[:, at:at + heads] + acc[:, at + LANES + heads:at + LANES + 2 * heads] + bias
    dtn[...] = jnp.maximum(dt_sum, 0.0) + jnp.log1p(jnp.exp(-jnp.abs(dt_sum)))
    x_load.wait()
    local_states(False, dims, len_ref, xv, bn, dtn, decay_ref, work, *kept[0][2:])
    exchange(0)
    combine(0)
    block(False, 0)
    for back in range(2):
        kx_copy(back).wait_recv()

    def tick(t, _):
        for back in range(2):
            i = t - ((nz - 1 - zpos) if back else zpos) * Z_LAG

            @pl.when((i >= 0) & (i < half_pairs))
            def _(back=back, i=i):
                relay(back, i)

            late = i - CORE_LAG

            @pl.when((late >= 0) & (late < half_pairs))
            def _(back=back, late=late):
                settle(back, late)

        return 0

    lax.fori_loop(0, half_pairs + CORE_LAG + (nz - 1) * Z_LAG, tick, 0)

    for j in range(2):
        cross(j).wait_send()
    for k in range(1, half_ring + 1):
        for d in range(2):
            for j in range(4):
                if k <= full or (j < 2) == (d == 0):
                    ring(d, k, j).wait_send()
    for u in range(far + 1):
        for j in range(4):
            side(u, j).wait_send()
    for back in range(2):
        remote(kv[back], ksib[back], k_s.at[back], k_r.at[back], seq=partner).wait_send()
        kx_copy(back).wait_send()

        def drain(i, _, back=back):
            remote(lout[back].at[i], lin[back].at[i], l_s.at[back, i], l_r.at[back, i], seq=partner).wait_send()
            x_copy(back, i).wait_send()
            e_copy(back, i).wait_send()

            @pl.when(zpos != (0 if back else nz - 1))
            def _():
                z_copy(back, i).wait_send()

            out_copy(back, i).wait()
            out_copy(back, half_pairs + i).wait()
            return 0

        lax.fori_loop(0, half_pairs, drain, 0)


def fused(hidden, values, seg_next, proj_bc, proj_dt, dt_bias, decay_rate, skip_gain,
          bc_prev, dt_prev, seg_prev, grad, gw):
    count = lax.axis_size("seq")
    tokens, heads = dt_prev.shape
    width = values.shape[1]
    dims = (tokens // SPAN, heads, gw // LANES, width // heads)
    npair = width // LANES
    half_pairs = npair // 2
    n = count // 2
    f32, bf16 = jnp.float32, jnp.bfloat16
    dma = pltpu.SemaphoreType.DMA
    wrows = proj_bc.shape[0]
    packed = wrows + LANES * LANES // (2 * gw)
    nblocks = dims[0]
    work = [pltpu.VMEM((tokens, heads), f32), pltpu.VMEM((nblocks, heads, SPAN), f32),
            pltpu.VMEM((nblocks, heads, SPAN), f32), pltpu.VMEM((tokens, heads), f32)]
    kept = [pltpu.VMEM(s, f32) for s in ((npair, tokens, LANES), (npair, tokens, LANES),
                                         (nblocks + 1, npair, LANES, LANES), (nblocks + 1, npair, 1, LANES))]
    box = [pltpu.VMEM((half_pairs, LANES, LANES), bf16)] * 2
    gain = [pltpu.VMEM((npair, LANES), f32)] * 2
    half_gain = [pltpu.VMEM((half_pairs, LANES), f32)] * 2
    hbm = pl.BlockSpec(memory_space=pl.ANY)
    steps = n // 2
    return pl.pallas_call(
        functools.partial(fused_kernel, count, dims),
        out_shape=[jax.ShapeDtypeStruct(values.shape, bf16)] * 2,
        in_specs=[SM] * 2 + [VM] * 5 + [hbm] * 5,
        out_specs=[hbm] * 2,
        scratch_shapes=[
            pltpu.VMEM((tokens, hidden.shape[1]), bf16),
            pltpu.VMEM((n, 4, packed, 2 * gw), bf16),
            pltpu.VMEM((packed, 2 * gw), bf16),
            pltpu.VMEM((tokens, width), bf16), pltpu.VMEM((tokens, width), bf16),
            *[pltpu.VMEM((tokens, gw), bf16)] * 4,
            pltpu.VMEM((tokens, 2 * gw + 2 * LANES), f32),
            pltpu.VMEM((tokens, heads), f32), pltpu.VMEM((tokens, heads), f32),
            pltpu.VMEM((1, heads), f32), pltpu.VMEM((1, heads), f32),
            *work, *work, *kept, *kept, *box * 8, *gain * 2, *half_gain * 2,
            dma((9,)), dma((2, steps, 4)), dma((2, steps, 4)), dma((n, 4)), dma((n, 4)),
            dma((2,)), dma((2,)), dma((2, half_pairs)), dma((2, half_pairs)), dma((4,)), dma((4,)),
            dma((2, half_pairs)), dma((2, half_pairs)), dma((2, half_pairs)), dma((2, half_pairs)),
            dma((2, half_pairs)), dma((2, half_pairs)), dma((2, npair)),
        ],
        compiler_params=pltpu.CompilerParams(
            collective_id=2, has_side_effects=True, vmem_limit_bytes=67_043_328),
        name="fused",
    )(seg_next, seg_prev, dt_bias[None], decay_rate[None], skip_gain[None], proj_dt, dt_prev.T,
      hidden, values, proj_bc, bc_prev, grad)


def body(
    hidden_next, values_next, seg_next, proj_bc, proj_dt, dt_bias, decay_rate, skip_gain,
    bc_prev, dt_prev, seg_prev, grad_prev,
):
    tokens_dev = hidden_next.shape[0]
    bc_width = proj_bc.shape[1]
    heads_all = proj_dt.shape[1]
    fsdp_count = lax.axis_size("fsdp")
    fsdp_place = lax.axis_index("fsdp")
    seq_count = lax.axis_size("seq")
    heads_dev = heads_all // fsdp_count
    state_dim = bc_width // (2 * GW)
    per_group = heads_all // GW
    groups_dev = max(1, heads_dev // per_group)
    first_head = fsdp_place * heads_dev
    first_group = first_head // per_group
    rows_dev = proj_bc.shape[0]
    half = bc_width // 2
    gw = groups_dev * state_dim

    if fsdp_count == 2 and seq_count % 4 == 0 and seq_count >= 8 and heads_all == LANES \
            and rows_dev == 2 * LANES and groups_dev * per_group == heads_dev:
        return fused(hidden_next, values_next, seg_next, proj_bc, proj_dt, dt_bias, decay_rate,
                     skip_gain, bc_prev, dt_prev, seg_prev, grad_prev, gw)

    blocks = []
    for f in range(fsdp_count):
        g0 = (f * heads_dev // per_group) * state_dim
        blocks.append([proj_bc[:, g0:g0 + gw], proj_bc[:, half + g0:half + g0 + gw]])
    ring = fsdp_count == 2 and seq_count % 4 == 0 and rows_dev % (2 * LANES) == 0 and heads_all == LANES
    if ring:
        shard = jnp.concatenate([*blocks[0], *blocks[1], proj_dt], axis=1)
        bc_next, dt_sum = gathered_sums(hidden_next, shard, 2 * gw)
        dt_sum = lax.dynamic_slice_in_dim(dt_sum, first_head, heads_dev, 1)
    else:
        pieces = []
        for f in range(fsdp_count):
            pieces += [*blocks[f], proj_dt[:, f * heads_dev:(f + 1) * heads_dev]]
        weights = lax.all_gather(jnp.concatenate(pieces, axis=1), "seq", axis=0, tiled=True)
        owned = lax.dynamic_slice_in_dim(
            hidden_next.reshape(tokens_dev, seq_count, fsdp_count, rows_dev), fsdp_place, 1, 2
        ).reshape(tokens_dev, seq_count * rows_dev)
        sums = lax.psum_scatter(jnp.dot(owned, weights, preferred_element_type=jnp.float32),
                                "fsdp", scatter_dimension=1, tiled=True)
        bc_next, dt_sum = sums[:, :2 * gw].astype(jnp.bfloat16), sums[:, 2 * gw:]

    decay = lax.dynamic_slice_in_dim(decay_rate, first_head, heads_dev, 0)[None]
    skip = lax.dynamic_slice_in_dim(skip_gain, first_head, heads_dev, 0)[None]
    bias = lax.dynamic_slice_in_dim(dt_bias, first_head, heads_dev, 0)[None]

    b_prev = lax.dynamic_slice_in_dim(bc_prev, first_group * state_dim, gw, 1)
    c_prev = lax.dynamic_slice_in_dim(bc_prev, half + first_group * state_dim, gw, 1)
    b_next, c_next = bc_next[:, :gw], bc_next[:, gw:]
    dt_next = jax.nn.softplus(dt_sum + bias)
    out_next, grad_values = chains(
        seg_next, values_next, c_next, b_next, dt_next, decay, skip,
        seg_prev, grad_prev, b_prev, c_prev, dt_prev)
    return (out_next, grad_values)


def solution(mesh):
    in_specs = (
        P("seq", None), P("seq", "fsdp"), P(), P(("seq", "fsdp"), None), P(("seq", "fsdp"), None),
        P(), P(), P(), P("seq", None), P("seq", "fsdp"), P(), P("seq", "fsdp"),
    )
    out_specs = (P("seq", "fsdp"), P("seq", "fsdp"))
    return jax.shard_map(body, mesh=mesh, in_specs=in_specs, out_specs=out_specs, check_vma=False)
```

```python
import functools

import jax
import jax.numpy as jnp
from jax import lax
from jax.experimental import pallas as pl
from jax.experimental.pallas import tpu as pltpu
from jax.sharding import PartitionSpec as P

GW = 4
SPAN = 128
LANES = 128
MESH = pl.DeviceIdType.MESH


def widen(a, c, head_dim):
    per = LANES // head_dim
    lane = lax.broadcasted_iota(jnp.int32, (1, LANES), 1)
    res = a[:, c * per:c * per + 1]
    for k in range(1, per):
        res = jnp.where(lane >= k * head_dim, a[:, c * per + k:c * per + k + 1], res)
    return jnp.broadcast_to(res, (a.shape[0], LANES))


def seg_maker(len_ref):
    bound = []
    total = jnp.int32(0)
    for k in range(len_ref.shape[0] - 1):
        total = total + len_ref[k]
        bound.append(total)

    def seg_of(pos):
        s = jnp.zeros_like(pos)
        for b in bound:
            s = s + (b <= pos).astype(jnp.int32)
        return s

    return seg_of


def local_states(back, dims, len_ref, x_ref, q_ref, dt_ref, decay_ref, work, pre, keep):
    nblocks, heads, groups, head_dim = dims
    cum_s, cum_t, dt_t, fout_s = work
    npair = heads * head_dim // LANES
    pair_group = npair // groups
    seg_of = seg_maker(len_ref)
    slab = lax.axis_index("seq") * (nblocks * SPAN)
    dim0 = lax.broadcasted_iota(jnp.int32, (SPAN, SPAN), 0)
    dim1 = lax.broadcasted_iota(jnp.int32, (SPAN, SPAN), 1)
    tril = (dim0 >= dim1).astype(jnp.float32)
    for c in range(npair):
        pre[0, c] = jnp.zeros((LANES, LANES), jnp.float32)
        keep[0, c] = jnp.ones((1, LANES), jnp.float32)
    for step in range(nblocks):
        b = nblocks - 1 - step if back else step
        rows = slice(b * SPAN, (b + 1) * SPAN)
        dt = dt_ref[rows, :]
        cum = jnp.dot(tril, -(dt * decay_ref[...]), precision=lax.Precision.HIGHEST,
                      preferred_element_type=jnp.float32)
        end = cum[SPAN - 1:SPAN, :]
        cum_s[rows, :] = cum
        cum_t[b] = cum.T
        dt_t[b] = dt.T
        seg = seg_of(slab + b * SPAN + lax.broadcasted_iota(jnp.int32, (SPAN, heads), 0))
        edge = slab + b * SPAN + lax.broadcasted_iota(jnp.int32, (1, heads), 0) * 0
        seg_e = seg_of(edge + (SPAN - 1))
        seg_b = jnp.where(edge == 0, 0, seg_of(edge - 1))
        send = jnp.where(seg == seg_e, jnp.exp(end - cum), 0.0) * dt
        read = jnp.where(seg == seg_b, jnp.exp(cum), 0.0)
        carry = jnp.where(seg_e == seg_b, jnp.exp(end), 0.0)
        f_in = read if back else send
        fout_s[rows, :] = send if back else read
        qt = [q_ref[rows, g * LANES:(g + 1) * LANES].T for g in range(groups)]
        for c in range(npair):
            cols = slice(c * LANES, (c + 1) * LANES)
            sent = (x_ref[rows, cols].astype(jnp.float32) * widen(f_in, c, head_dim)).astype(jnp.bfloat16)
            loc = jnp.dot(qt[c // pair_group], sent, preferred_element_type=jnp.float32)
            wide = widen(carry, c, head_dim)
            pre[step + 1, c] = wide * pre[step, c] + loc
            keep[step + 1, c] = wide * keep[step, c]


def in_block(back, dims, len_ref, x_ref, p_ref, q_ref, dt_ref, skip_ref, work, inside, fexp, span=None):
    nblocks, heads, groups, head_dim = dims
    cum_s, cum_t, dt_t, fout_s = work
    npair = heads * head_dim // LANES
    per = LANES // head_dim
    pair_group = npair // groups
    seg_of = seg_maker(len_ref)
    slab = lax.axis_index("seq") * (nblocks * SPAN)
    dim0 = lax.broadcasted_iota(jnp.int32, (SPAN, SPAN), 0)
    dim1 = lax.broadcasted_iota(jnp.int32, (SPAN, SPAN), 1)
    lane = lax.broadcasted_iota(jnp.int32, (1, LANES), 1)

    def one(b, _):
        start = pl.multiple_of(b * SPAN, SPAN)
        rows = pl.ds(start, SPAN)
        seg_i = seg_of(slab + start + dim0)
        seg_j = seg_of(slab + start + dim1)
        order = (dim1 >= dim0) if back else (dim1 <= dim0)
        bias = jnp.where((seg_i == seg_j) & order, 0.0, -jnp.inf)
        cum = cum_s[rows, :]
        dt = dt_ref[rows, :]
        f_out = fout_s[rows, :]
        for g in range(groups):
            gl = slice(g * LANES, (g + 1) * LANES)
            score = lax.dot_general(p_ref[rows, gl], q_ref[rows, gl], (((1,), (1,)), ((), ())),
                                    preferred_element_type=jnp.float32)
            for c in range(g * pair_group, (g + 1) * pair_group):
                cols = slice(c * LANES, (c + 1) * LANES)
                x = x_ref[rows, cols]
                mixes, parts = [], []
                for k in range(per):
                    h = c * per + k
                    col = cum[:, h:h + 1]
                    row = cum_t[b, h:h + 1, :]
                    spread = (row - col) if back else (col - row)
                    w = jnp.exp(spread + bias) * score
                    if not back:
                        w = w * dt_t[b, h:h + 1, :]
                    mixes.append(w.astype(jnp.bfloat16))
                    mine = (lane >= k * head_dim) & (lane < (k + 1) * head_dim)
                    parts.append(jnp.where(mine, x, jnp.zeros_like(x)))
                acc = jnp.dot(jnp.concatenate(mixes, 1), jnp.concatenate(parts, 0),
                              preferred_element_type=jnp.float32)
                if back:
                    acc = acc * widen(dt, c, head_dim)
                inside[c, rows, :] = acc + widen(skip_ref[...], c, head_dim) * x.astype(jnp.float32)
                fexp[c, rows, :] = widen(f_out, c, head_dim)
        return 0

    first, last = (0, nblocks) if span is None else span
    lax.fori_loop(first, last, one, 0)


HOP_CHUNKS = 5


def chain_kernel(count, dims, len_ref, x_ref, p_ref, q_ref, dt_ref, decay_ref, skip_ref,
                 lenb_ref, xb_ref, pb_ref, qb_ref, dtb_ref,
                 out_ref, grad_ref, *scratch):
    work, work_b, rest = scratch[:4], scratch[4:8], scratch[12:]
    inside_b, fexp_b, pre_b, keep_b = scratch[8:12]
    inside, fexp, pre, keep, inbox, outbox, in_b, out_b, s_sem, r_sem, sb_sem, rb_sem = rest
    nblocks, heads, groups, head_dim = dims
    npair = heads * head_dim // LANES
    pair_group = npair // groups
    me = lax.axis_index("seq")
    low, high = me == 0, me == count - 1

    barrier = pltpu.get_barrier_semaphore()

    @pl.when(jnp.logical_not(low))
    def _():
        pl.semaphore_signal(barrier, inc=1, device_id={"seq": me - 1}, device_id_type=MESH)

    @pl.when(jnp.logical_not(high))
    def _():
        pl.semaphore_signal(barrier, inc=1, device_id={"seq": me + 1}, device_id_type=MESH)

    local_states(False, dims, len_ref, x_ref, q_ref, dt_ref, decay_ref, work, pre, keep)
    local_states(True, dims, lenb_ref, xb_ref, qb_ref, dtb_ref, decay_ref, work_b, pre_b, keep_b)

    @pl.when(low)
    def _():
        inbox[...] = jnp.zeros_like(inbox)

    @pl.when(high)
    def _():
        in_b[...] = jnp.zeros_like(in_b)

    pl.semaphore_wait(barrier, jnp.where(low, 0, 1) + jnp.where(high, 0, 1))

    def hop(back, c):
        return pltpu.make_async_remote_copy(
            src_ref=(out_b if back else outbox).at[c], dst_ref=(in_b if back else inbox).at[c],
            send_sem=(sb_sem if back else s_sem).at[c], recv_sem=(rb_sem if back else r_sem).at[c],
            device_id={"seq": me - 1 if back else me + 1}, device_id_type=MESH)

    def relay(back, c):
        first, last = (high, low) if back else (low, high)
        kp, pr = (keep_b, pre_b) if back else (keep, pre)

        @pl.when(jnp.logical_not(first))
        def _():
            hop(back, c).wait_recv()

        @pl.when(jnp.logical_not(last))
        def _():
            state = (in_b if back else inbox)[c].astype(jnp.float32)
            (out_b if back else outbox)[c] = (kp[nblocks, c] * state + pr[nblocks, c]).astype(jnp.bfloat16)
            hop(back, c).start()

    def finish(back, c):
        kp, pr, ins, fx, vec, out = (
            (keep_b, pre_b, inside_b, fexp_b, pb_ref, grad_ref) if back
            else (keep, pre, inside, fexp, p_ref, out_ref))
        g = c // pair_group
        cols = pl.ds(pl.multiple_of(c * LANES, LANES), LANES)
        gl = pl.ds(pl.multiple_of(g * LANES, LANES), LANES)
        state = (in_b if back else inbox)[c].astype(jnp.float32)
        for step in range(nblocks):
            b = nblocks - 1 - step if back else step
            rows = slice(b * SPAN, (b + 1) * SPAN)
            entering = (kp[step, c] * state + pr[step, c]).astype(jnp.bfloat16)
            y = jnp.dot(vec[rows, gl], entering, preferred_element_type=jnp.float32)
            out[rows, cols] = (ins[c, rows, :] + fx[c, rows, :] * y).astype(jnp.bfloat16)

    lag = (2 * me - (count - 1)) * HOP_CHUNKS
    up_first = lag < 0
    gap = jnp.where(up_first, -lag, lag)
    block_at = jnp.where(gap >= npair, npair, 0)

    def step_of(i, _):
        @pl.when(i == block_at)
        def _():
            in_block(False, dims, len_ref, x_ref, p_ref, q_ref, dt_ref, skip_ref, work, inside, fexp)
            in_block(True, dims, lenb_ref, xb_ref, pb_ref, qb_ref, dtb_ref, skip_ref, work_b, inside_b, fexp_b)

        for back in (False, True):
            leads = jnp.logical_not(up_first) if back else up_first
            c = i - jnp.where(leads, 0, gap)

            @pl.when((c >= 0) & (c < npair))
            def _(back=back, c=c):
                relay(back, c)

            done = jnp.where(leads, i - npair, c)

            @pl.when((done >= 0) & (done < npair))
            def _(back=back, done=done):
                finish(back, done)

        return 0

    lax.fori_loop(0, npair + jnp.maximum(gap, npair), step_of, 0)

    def drain(c, _):
        @pl.when(jnp.logical_not(high))
        def _():
            hop(False, c).wait_send()

        @pl.when(jnp.logical_not(low))
        def _():
            hop(True, c).wait_send()

        return 0

    lax.fori_loop(0, npair, drain, 0)


def sizes_of(x, p_vec, dt):
    tokens, width = x.shape
    heads = dt.shape[1]
    dims = (tokens // SPAN, heads, p_vec.shape[1] // LANES, width // heads)
    nblocks, npair = dims[0], width // LANES
    f32 = jnp.float32
    work = [pltpu.VMEM((tokens, heads), f32), pltpu.VMEM((nblocks, heads, SPAN), f32),
            pltpu.VMEM((nblocks, heads, SPAN), f32), pltpu.VMEM((tokens, heads), f32)]
    kept = [(npair, tokens, LANES), (npair, tokens, LANES),
            (nblocks + 1, npair, LANES, LANES), (nblocks + 1, npair, 1, LANES)]
    return dims, npair, work, kept


VM = pl.BlockSpec(memory_space=pltpu.VMEM)
SM = pl.BlockSpec(memory_space=pltpu.SMEM)


def chains(lengths, x, p_vec, q_vec, dt, decay, skip, *back):
    dims, npair, work, kept = sizes_of(x, p_vec, dt)
    box = pltpu.VMEM((npair, LANES, LANES), jnp.bfloat16)
    sem = pltpu.SemaphoreType.DMA((npair,))
    return pl.pallas_call(
        functools.partial(chain_kernel, lax.axis_size("seq"), dims),
        out_shape=[jax.ShapeDtypeStruct(x.shape, jnp.bfloat16)] * 2,
        in_specs=[SM] + [VM] * 6 + [SM] + [VM] * 4,
        out_specs=[VM] * 2,
        scratch_shapes=(work * 2 + [pltpu.VMEM(k, jnp.float32) for k in kept] * 2
                        + [box] * 4 + [sem] * 4),
        compiler_params=pltpu.CompilerParams(
            collective_id=0, has_side_effects=True, vmem_limit_bytes=56 * 1024 * 1024),
        cost_estimate=pl.CostEstimate(flops=40_000_000_000, bytes_accessed=40_000_000, transcendentals=0),
        name="chains",
    )(lengths, x, p_vec, q_vec, dt, decay, skip, *back)


PIECES = 4


def gather_kernel(count, h_ref, w_ref, bc_ref, dt_ref,
                  held, acc, bc_out, bc_in, dt_out, dt_in,
                  ring_s, ring_r, side_s, side_r, x_s, x_r):
    me, f = lax.axis_index("seq"), lax.axis_index("fsdp")
    n = count // 2
    half_ring = n // 2
    core, chip = me % 2, me // 2
    r = jnp.where(chip % 2 == 0, chip // 2, n - 1 - chip // 2)
    rows = w_ref.shape[0]
    piece = rows // PIECES
    wide = bc_ref.shape[1]

    def id_of(pos, which):
        p = (pos + 2 * n) % n
        up = p < half_ring
        return jnp.where(up, p * 2, (n - 1 - p) * 2 + 1) * 2 + which

    nxt, prv, partner = id_of(r + 1, core), id_of(r - 1, core), chip * 2 + 1 - core

    barrier = pltpu.get_barrier_semaphore()
    for peer in (nxt, prv, partner):
        pl.semaphore_signal(barrier, inc=1, device_id={"seq": peer}, device_id_type=MESH)
    pl.semaphore_signal(barrier, inc=1, device_id={"fsdp": 1 - f}, device_id_type=MESH)
    pl.semaphore_wait(barrier, 4)

    def part(p):
        return pl.ds(p * piece, piece)

    def origin(step, p, which):
        return id_of(r - step if p < PIECES // 2 else r + step, which)

    def ring_copy(step, p, src):
        return pltpu.make_async_remote_copy(
            src_ref=src, dst_ref=held.at[origin(step, p, core), part(p), :],
            send_sem=ring_s.at[step, p], recv_sem=ring_r.at[step, p],
            device_id={"seq": nxt if p < PIECES // 2 else prv}, device_id_type=MESH)

    def side_copy(step, p, src):
        return pltpu.make_async_remote_copy(
            src_ref=src, dst_ref=held.at[origin(step, p, core), part(p), :],
            send_sem=side_s.at[step, p], recv_sem=side_r.at[step, p],
            device_id={"seq": partner}, device_id_type=MESH)

    def landed(step, p):
        return held.at[origin(step, p, core), part(p), :]

    for p in range(PIECES):
        ring_copy(0, p, w_ref.at[part(p), :]).start()
    for p in range(PIECES):
        side_copy(0, p, w_ref.at[part(p), :]).start()

    def columns(seq_index, first):
        start = (seq_index * 2 + f) * rows + first
        return h_ref[:, pl.ds(pl.multiple_of(start, rows // 2), rows // 2)]

    def mac(step, which):
        half = rows // 2
        lo, hi = origin(step, 0, which), origin(step, PIECES - 1, which)
        left = jnp.concatenate([columns(lo, 0), columns(hi, half)], axis=1)
        right = jnp.concatenate([held[lo, 0:half, :], held[hi, half:, :]], axis=0)
        acc[...] += jnp.dot(left, right, preferred_element_type=jnp.float32)

    acc[...] = jnp.dot(jnp.concatenate([columns(me, 0), columns(me, rows // 2)], axis=1), w_ref[...],
                       preferred_element_type=jnp.float32)

    def one(step, _):
        for p in (0, PIECES // 2, 1, PIECES // 2 + 1):
            ring_copy(step, p, landed(step, p)).wait_recv()

            @pl.when(step < n - 2)
            def _(p=p):
                ring_copy(step + 1, p, landed(step + 1, p)).start()

            side_copy(step + 1, p, landed(step + 1, p)).start()
        mac(step + 1, core)
        for p in range(PIECES):
            side_copy(step, p, landed(step, p)).wait_recv()
        mac(step, 1 - core)
        return 0

    lax.fori_loop(0, n - 1, one, 0)
    for p in range(PIECES):
        side_copy(n - 1, p, landed(n - 1, p)).wait_recv()
    mac(n - 1, 1 - core)

    def cross(src, dst, k):
        return pltpu.make_async_remote_copy(
            src_ref=src, dst_ref=dst, send_sem=x_s.at[k], recv_sem=x_r.at[k],
            device_id={"fsdp": 1 - f}, device_id_type=MESH)

    def side_of(which):
        return pl.ds(pl.multiple_of(which * wide, wide), wide)

    bc_out[...] = acc[:, side_of(1 - f)]
    dt_out[...] = acc[:, 2 * wide:]
    cross(bc_out, bc_in, 0).start()
    cross(dt_out, dt_in, 1).start()

    def drain(step, _):
        for p in range(PIECES):
            @pl.when(step < n - 1)
            def _(p=p):
                ring_copy(step, p, landed(step, p)).wait_send()

            side_copy(step, p, landed(step, p)).wait_send()
        return 0

    lax.fori_loop(0, n, drain, 0)
    cross(bc_out, bc_in, 0).wait()
    bc_ref[...] = (acc[:, side_of(f)] + bc_in[...]).astype(jnp.bfloat16)
    cross(dt_out, dt_in, 1).wait()
    dt_ref[...] = acc[:, 2 * wide:] + dt_in[...]


def gathered_sums(hidden, shard, wide):
    count = lax.axis_size("seq")
    tokens, total = hidden.shape[0], shard.shape[1]
    f32, bf16 = jnp.float32, jnp.bfloat16
    n = count // 2
    dma = pltpu.SemaphoreType.DMA
    return pl.pallas_call(
        functools.partial(gather_kernel, count),
        out_shape=[jax.ShapeDtypeStruct((tokens, wide), bf16),
                   jax.ShapeDtypeStruct((tokens, total - 2 * wide), f32)],
        in_specs=[VM] * 2,
        out_specs=[VM] * 2,
        scratch_shapes=[
            pltpu.VMEM((count,) + shard.shape, bf16),
            pltpu.VMEM((tokens, total), f32),
            pltpu.VMEM((tokens, wide), f32), pltpu.VMEM((tokens, wide), f32),
            pltpu.VMEM((tokens, total - 2 * wide), f32), pltpu.VMEM((tokens, total - 2 * wide), f32),
            dma((n, PIECES)), dma((n, PIECES)), dma((n, PIECES)), dma((n, PIECES)), dma((2,)), dma((2,)),
        ],
        compiler_params=pltpu.CompilerParams(
            collective_id=1, has_side_effects=True, vmem_limit_bytes=32 * 1024 * 1024),
        cost_estimate=pl.CostEstimate(flops=40_000_000_000, bytes_accessed=40_000_000, transcendentals=0),
        name="gather_project",
    )(hidden, shard)


Z_LAG = 4
CORE_LAG = 3
BATCH = 4
EARLY = 6


def fused_kernel(count, dims, len_ref, lenb_ref, bias_in, decay_in, skip_in, pdt_ref, dtt_ref,
                 h_hbm, x_hbm, w_hbm, bcp_hbm, g_hbm, out_hbm, grad_hbm,
                 hid, held_b, held_c, yout_b, yout_c, xv, gv, bp, cp, bn, cn, acc, dtn, dtp, decay_ref, skip_ref,
                 *scratch):
    work, work_b = scratch[:4], scratch[4:8]
    kept = (scratch[8:12], scratch[12:16])
    lout, lin, xout, xin, zout, zin, eout, ein, eown, kv, ksib, kxo, kxi = (
        (scratch[16 + 2 * i], scratch[17 + 2 * i]) for i in range(13))
    (ld, ring_s, ring_r, side_s, side_r, y_s, y_r, l_s, l_r, k_s, k_r, c_s, c_r, z_s, z_r,
     e_s, e_r, o_sem) = scratch[42:]
    nblocks, heads, groups, head_dim = dims
    npair = heads * head_dim // LANES
    pair_group = npair // groups
    half_pairs = npair // 2
    me, f = lax.axis_index("seq"), lax.axis_index("fsdp")
    core, chip = me % 2, me // 2
    xpos, zpos, nz = chip % 2, chip // 2, count // 4
    n = count // 2
    half_ring = n // 2
    full = half_ring - 1
    far = 2 * full + 1
    gw = groups * LANES
    wrows = w_hbm.shape[0]
    r = jnp.where(xpos == 0, zpos, n - 1 - zpos)

    def chip_at(pos):
        p = (pos + 2 * n) % n
        return jnp.where(p < half_ring, p * 2, (n - 1 - p) * 2 + 1)

    nxt, prv = chip_at(r + 1) * 2 + core, chip_at(r - 1) * 2 + core
    partner = chip * 2 + 1 - core
    xpeer = (zpos * 2 + 1 - xpos) * 2 + core
    own, other = core * 2 + f, core * 2 + 1 - f

    def at_cols(start):
        return pl.ds(pl.multiple_of(start, LANES), gw)

    def load(src, dst, k):
        return pltpu.make_async_copy(src, dst, ld.at[k])

    w_half = w_hbm.shape[1] // 2
    w_loads = [
        load(w_hbm.at[:, at_cols(f * gw)], held_b.at[chip, own, 0:wrows, :], 0),
        load(w_hbm.at[:, at_cols((1 - f) * gw)], yout_b.at[0:wrows, :], 1),
        load(w_hbm.at[:, at_cols(w_half + f * gw)], held_c.at[chip, own, :, :], 2),
        load(w_hbm.at[:, at_cols(w_half + (1 - f) * gw)], yout_c, 3),
    ]
    b_loads = [
        load(g_hbm, gv, 4),
        load(bcp_hbm.at[:, at_cols(f * gw)], bp, 5),
        load(bcp_hbm.at[:, at_cols(w_half + f * gw)], cp, 6),
    ]
    h_load, x_load = load(h_hbm, hid, 7), load(x_hbm, xv, 8)
    for copy in (*w_loads, *b_loads, h_load, x_load):
        copy.start()

    barrier = pltpu.get_barrier_semaphore()
    for peer in (partner, xpeer):
        pl.semaphore_signal(barrier, inc=1, device_id={"seq": peer}, device_id_type=MESH)
    pl.semaphore_signal(barrier, inc=1, device_id={"fsdp": 1 - f}, device_id_type=MESH)

    @pl.when(zpos > 0)
    def _():
        pl.semaphore_signal(barrier, inc=1, device_id={"seq": me - 4}, device_id_type=MESH)

    @pl.when(zpos < nz - 1)
    def _():
        pl.semaphore_signal(barrier, inc=1, device_id={"seq": me + 4}, device_id_type=MESH)

    lane = lax.broadcasted_iota(jnp.int32, (LANES, LANES), 1)
    top = pdt_ref[0:LANES, :].astype(jnp.float32)
    low = pdt_ref[LANES:2 * LANES, :].astype(jnp.float32)
    pack0 = jnp.where(lane < heads, top, pltpu.roll(low, heads, 1))
    pack1 = jnp.where(lane < heads, pltpu.roll(top, heads, 1), low)
    mine = jnp.where(f == 0, pack0, pack1).astype(jnp.bfloat16)
    theirs = jnp.where(f == 0, pack1, pack0).astype(jnp.bfloat16)
    strips = gw // LANES
    strip = LANES // strips
    for k in range(strips):
        lanes = slice(k * LANES, (k + 1) * LANES)
        held_b[chip, own, wrows:wrows + strip, lanes] = mine[k * strip:(k + 1) * strip, :]
        yout_b[wrows:wrows + strip, lanes] = theirs[k * strip:(k + 1) * strip, :]
    decay_ref[...] = jnp.where(f == 0, decay_in[:, 0:heads], decay_in[:, heads:2 * heads])
    skip_ref[...] = jnp.where(f == 0, skip_in[:, 0:heads], skip_in[:, heads:2 * heads])
    bias = jnp.where(f == 0, bias_in[:, 0:heads], bias_in[:, heads:2 * heads])
    for b in range(nblocks):
        dtp[b * SPAN:(b + 1) * SPAN, :] = dtt_ref[:, b * SPAN:(b + 1) * SPAN].T

    pl.semaphore_wait(barrier, 3 + jnp.where(zpos > 0, 1, 0) + jnp.where(zpos < nz - 1, 1, 0))
    for copy in w_loads:
        copy.wait()

    def piece(where, j, mine=True):
        base = (core if mine else 1 - core) * 2
        return (held_b if j < 2 else held_c).at[where, base + (f if j % 2 == 0 else 1 - f)]

    def remote(src, dst, s, rv, **peer):
        return pltpu.make_async_remote_copy(src_ref=src, dst_ref=dst, send_sem=s, recv_sem=rv,
                                            device_id=peer, device_id_type=MESH)

    def ring(d, k, j, arrived=False):
        away = k if arrived else k - 1
        ref = piece(chip_at(r - away if d == 0 else r + away), j)
        return remote(ref, ref, ring_s.at[d, k - 1, j], ring_r.at[d, k - 1, j],
                      seq=nxt if d == 0 else prv)

    def chip_of(u):
        return chip_at(r - u if u <= full else (r + (u - full) if u < far else r + half_ring))

    def side(u, j, arrived=False):
        ref = piece(chip_of(u), j, not arrived)
        return remote(ref, ref, side_s.at[u, j], side_r.at[u, j], seq=partner)

    def cross(kind, arrived=False):
        ref = held_c if kind else held_b
        return remote(yout_c if kind else yout_b, ref.at[chip, other if arrived else own],
                      y_s.at[kind], y_r.at[kind], fsdp=1 - f)

    def begin(j):
        ring(0, 1, j).start()
        ring(1, 1, j).start()
        side(0, j).start()

    for kind in range(2):
        cross(kind).start()
        begin(2 * kind)

    def receive(k, kind, second=False):
        for d in range(2):
            if k > full and second:
                continue
            j = 2 * kind + ((1 - d if second else d) if k > 1 or kind else int(second))
            ring(d, k, j, True).wait_recv()
            if k < full or (k == full and j % 2 == d):
                ring(d, k + 1, j).start()
            side(far if k > full else (k if d == 0 else full + k), j).start()

    wide = 4 * wrows

    def add(at, value, first):
        cols = slice(at, at + value.shape[1])
        acc[:, cols] = value if first else acc[:, cols] + value

    def mac(u, kind, first=False):
        for j in (2 * kind, 2 * kind + 1):
            side(u, j, True).wait_recv()
        q = chip_of(u)
        left = hid[:, pl.ds(pl.multiple_of(q * wide, wide), wide)]
        ref = held_c if kind else held_b
        add(gw + 2 * LANES if kind else 0,
            jnp.dot(left, jnp.concatenate([ref[q, s, 0:wrows, :] for s in range(4)], axis=0),
                    preferred_element_type=jnp.float32), first)
        if kind == 0:
            packs = jnp.concatenate(
                [held_b[q, s, wrows:wrows + strip, k * LANES:(k + 1) * LANES]
                 for s in range(4) for k in range(strips)], axis=0)
            for o in range(2):
                part = jnp.concatenate(
                    [left[:, s * wrows + o * LANES:s * wrows + (o + 1) * LANES] for s in range(4)], axis=1)
                add(gw + o * LANES, jnp.dot(part, packs, preferred_element_type=jnp.float32), first)

    def exchange(back):
        pre, keep = kept[back][2:]
        for c in range(npair):
            kv[back][c:c + 1, :] = keep[nblocks, c]
        remote(kv[back], ksib[back], k_s.at[back], k_r.at[back], seq=partner).start()

        def put(i, _):
            lout[back][i] = pre[nblocks, (1 - core) * half_pairs + i].astype(jnp.bfloat16)
            remote(lout[back].at[i], lin[back].at[i], l_s.at[back, i], l_r.at[back, i], seq=partner).start()
            return 0

        lax.fori_loop(0, half_pairs, put, 0)

    def lead_core(back):
        return (core == 1) if back else (core == 0)

    def lead_x(back):
        return (xpos == 1) if back else (xpos == 0)

    def ends(back):
        return (zpos == 0) if back else (zpos == nz - 1)

    def gives(back):
        return jnp.logical_not(ends(back)) | lead_x(back)

    def takes(back):
        return jnp.logical_not(ends(back) & lead_x(back))

    def row(ref, i):
        return ref[pl.ds(i, 1), :]

    def x_copy(back, i):
        return remote(xout[back].at[i], xin[back].at[i], c_s.at[back, i], c_r.at[back, i], seq=xpeer)

    def kx_copy(back):
        return remote(kxo[back], kxi[back], k_s.at[2 + back], k_r.at[2 + back], seq=xpeer)

    def combine(back):
        rows = pl.ds(pl.multiple_of(core * half_pairs, half_pairs), half_pairs)
        remote(kv[back], ksib[back], k_s.at[back], k_r.at[back], seq=partner).wait_recv()
        kxo[back][...] = kv[back][rows, :] * ksib[back][rows, :]
        sends = gives(back)

        @pl.when(sends)
        def _():
            kx_copy(back).start()

    def combine_part(back, start, stop):
        pre = kept[back][2]
        sends = gives(back)

        def put(i, _):
            g = core * half_pairs + i
            remote(lout[back].at[i], lin[back].at[i], l_s.at[back, i], l_r.at[back, i], seq=partner).wait_recv()
            lead = lead_core(back)
            total = (pre[nblocks, g] * jnp.where(lead, row(ksib[back], g), 1.0)
                     + lin[back][i].astype(jnp.float32) * jnp.where(lead, 1.0, row(kv[back], g)))
            xout[back][i] = total.astype(jnp.bfloat16)

            @pl.when(sends)
            def _():
                x_copy(back, i).start()

            return 0

        lax.fori_loop(start, stop, put, 0)

    def z_copy(back, i):
        return remote(zout[back].at[i], zin[back].at[i], z_s.at[back, i], z_r.at[back, i],
                      seq=me - 4 if back else me + 4)

    def e_copy(back, i):
        return remote(eout[back].at[i], ein[back].at[i], e_s.at[back, i], e_r.at[back, i], seq=partner)

    def out_copy(back, k):
        cols = pl.ds(pl.multiple_of(k * BATCH * LANES, LANES), BATCH * LANES)
        src, dst = (gv, grad_hbm) if back else (xv, out_hbm)
        return pltpu.make_async_copy(src.at[:, cols], dst.at[:, cols], o_sem.at[back, k])

    def finish(back, c0, states, i0):
        ins, fx, pre, keep = kept[back]
        vec, out = (bp, gv) if back else (cn, xv)
        gl = pl.ds(pl.multiple_of((c0 // pair_group) * LANES, LANES), LANES)
        for step in range(nblocks):
            b = nblocks - 1 - step if back else step
            rows = slice(b * SPAN, (b + 1) * SPAN)
            for k in range(0, BATCH, 2):
                entering = []
                for c, i in ((c0 + k, i0 + k), (c0 + k + 1, i0 + k + 1)):
                    state = states[i]
                    if step > 0:
                        state = (keep[step, c] * state.astype(jnp.float32) + pre[step, c]).astype(jnp.bfloat16)
                    entering.append(state)
                y = jnp.dot(vec[rows, gl], jnp.concatenate(entering, axis=1), preferred_element_type=jnp.float32)
                for m in range(2):
                    c = c0 + k + m
                    cols = pl.ds(pl.multiple_of(c * LANES, LANES), LANES)
                    part = y[:, m * LANES:(m + 1) * LANES]
                    out[rows, cols] = (ins[c, rows, :] + fx[c, rows, :] * part).astype(jnp.bfloat16)
        out_copy(back, c0 // BATCH).start()

    def relay(back, i):
        pre = kept[back][2]
        g = core * half_pairs + i
        z_first, z_last = (zpos == nz - 1, zpos == 0) if back else (zpos == 0, zpos == nz - 1)

        @pl.when(takes(back))
        def _():
            x_copy(back, i).wait_recv()

        @pl.when(jnp.logical_not(z_first))
        def _():
            z_copy(back, i).wait_recv()

        k_own, k_peer = row(kxo[back], i), row(kxi[back], i)
        l_own = xout[back][i].astype(jnp.float32)
        l_peer = jnp.where(takes(back), xin[back][i].astype(jnp.float32), 0.0)
        state = jnp.where(z_first, 0.0, zin[back][i].astype(jnp.float32))
        lead = lead_x(back)
        zout[back][i] = (k_own * k_peer * state + l_own * jnp.where(lead, k_peer, 1.0)
                         + l_peer * jnp.where(lead, 1.0, k_own)).astype(jnp.bfloat16)

        @pl.when(jnp.logical_not(z_last))
        def _():
            z_copy(back, i).start()

        state = jnp.where(lead, state, k_peer * state + l_peer)
        head = lead_core(back)
        k_lead = jnp.where(head, row(kv[back], g), row(ksib[back], g))
        l_lead = jnp.where(head, pre[nblocks, g], lin[back][i].astype(jnp.float32))
        after = k_lead * state + l_lead
        eout[back][i] = jnp.where(head, after, state).astype(jnp.bfloat16)
        e_copy(back, i).start()
        eown[back][i] = jnp.where(head, state, after).astype(jnp.bfloat16)

    def settle(back, i):
        for k in range(BATCH):
            e_copy(back, i + k).wait_recv()
        finish(back, core * half_pairs + i, eown[back], i)
        finish(back, (1 - core) * half_pairs + i, ein[back], i)

    def block(back, b):
        if back:
            in_block(True, dims, lenb_ref, gv, bp, cp, dtp, skip_ref, work_b, *kept[1][:2], span=(b, b + 1))
        else:
            in_block(False, dims, len_ref, xv, cn, bn, dtn, skip_ref, work, *kept[0][:2])

    for copy in b_loads:
        copy.wait()
    local_states(True, dims, lenb_ref, gv, cp, dtp, decay_ref, work_b, *kept[1][2:])
    for kind in range(2):
        cross(kind, True).wait_recv()
        begin(2 * kind + 1)
    receive(1, 0)
    exchange(1)
    block(True, 0)
    receive(1, 0, True)
    receive(1, 1)
    block(True, 1)
    h_load.wait()
    mac(0, 0, True)
    c_next = [(k, second) for k in range(1, full + 1) for second in (False, True)][1:]
    for k in range(2, full + 1):
        receive(k, 0)
        receive(k, 0, True)
        if k == 2:
            mac(0, 1, True)
        for u in (k - 1, full + k - 1):
            mac(u, 0)
        for _ in range(2 if k == full else 1):
            step, second = c_next.pop(0)
            receive(step, 1, second)
    for u in (full, 2 * full):
        mac(u, 0)
    receive(full + 1, 0)
    mac(far, 0)
    at = gw
    bn[...] = acc[:, 0:gw].astype(jnp.bfloat16)
    dt_sum = acc[:, at:at + heads] + acc[:, at + LANES + heads:at + LANES + 2 * heads] + bias
    dtn[...] = jnp.maximum(dt_sum, 0.0) + jnp.log1p(jnp.exp(-jnp.abs(dt_sum)))
    while len(c_next) > 1:
        step, second = c_next.pop(0)
        receive(step, 1, second)
    early = jnp.where(zpos == 0, EARLY, half_pairs)
    combine(1)
    combine_part(1, 0, early)
    x_load.wait()
    local_states(False, dims, len_ref, xv, bn, dtn, decay_ref, work, *kept[0][2:])
    exchange(0)
    for step, second in c_next:
        receive(step, 1, second)
    for k in range(1, full):
        for u in (k, full + k):
            mac(u, 1)
    combine(0)
    combine_part(0, 0, half_pairs)
    combine_part(1, early, half_pairs)
    for u in (full, 2 * full):
        mac(u, 1)
    receive(full + 1, 1)
    mac(far, 1)
    cn[...] = acc[:, gw + 2 * LANES:].astype(jnp.bfloat16)
    block(False, 0)
    for back in range(2):
        @pl.when(takes(back))
        def _(back=back):
            kx_copy(back).wait_recv()

        @pl.when(jnp.logical_not(takes(back)))
        def _(back=back):
            kxi[back][...] = jnp.zeros_like(kxi[back])


    def tick(t, _):
        for back in range(2):
            i = t - ((nz - 1 - zpos) if back else zpos) * Z_LAG

            @pl.when((i >= 0) & (i < half_pairs))
            def _(back=back, i=i):
                relay(back, i)

        for back in range(2):
            late = t - ((nz - 1 - zpos) if back else zpos) * Z_LAG - CORE_LAG

            @pl.when((late >= 0) & (late < half_pairs) & (late % BATCH == BATCH - 1))
            def _(back=back, late=late):
                settle(back, late - (BATCH - 1))

        return 0

    lax.fori_loop(0, half_pairs + CORE_LAG + (nz - 1) * Z_LAG, tick, 0)

    for j in range(2):
        cross(j).wait_send()
    for k in range(1, half_ring + 1):
        for d in range(2):
            for j in range(4):
                if k <= full or j % 2 == d:
                    ring(d, k, j).wait_send()
    for u in range(far + 1):
        for j in range(4):
            side(u, j).wait_send()
    for back in range(2):
        remote(kv[back], ksib[back], k_s.at[back], k_r.at[back], seq=partner).wait_send()
        given = gives(back)

        @pl.when(given)
        def _(back=back):
            kx_copy(back).wait_send()

        def drain(i, _, back=back, given=given):
            remote(lout[back].at[i], lin[back].at[i], l_s.at[back, i], l_r.at[back, i], seq=partner).wait_send()

            @pl.when(given)
            def _():
                x_copy(back, i).wait_send()

            e_copy(back, i).wait_send()

            @pl.when(zpos != (0 if back else nz - 1))
            def _():
                z_copy(back, i).wait_send()

            return 0

        lax.fori_loop(0, half_pairs, drain, 0)
        for k in range(npair // BATCH):
            out_copy(back, k).wait()


def fused(hidden, values, seg_next, proj_bc, proj_dt, dt_bias, decay_rate, skip_gain,
          bc_prev, dt_prev, seg_prev, grad, gw):
    count = lax.axis_size("seq")
    tokens, heads = dt_prev.shape
    width = values.shape[1]
    dims = (tokens // SPAN, heads, gw // LANES, width // heads)
    npair = width // LANES
    half_pairs = npair // 2
    n = count // 2
    f32, bf16 = jnp.float32, jnp.bfloat16
    dma = pltpu.SemaphoreType.DMA
    wrows = proj_bc.shape[0]
    packed = wrows + LANES * LANES // gw
    nblocks = dims[0]
    work = [pltpu.VMEM((tokens, heads), f32), pltpu.VMEM((nblocks, heads, SPAN), f32),
            pltpu.VMEM((nblocks, heads, SPAN), f32), pltpu.VMEM((tokens, heads), f32)]
    kept = [pltpu.VMEM(s, f32) for s in ((npair, tokens, LANES), (npair, tokens, LANES),
                                         (nblocks + 1, npair, LANES, LANES), (nblocks + 1, npair, 1, LANES))]
    box = [pltpu.VMEM((half_pairs, LANES, LANES), bf16)] * 2
    gain = [pltpu.VMEM((npair, LANES), f32)] * 2
    half_gain = [pltpu.VMEM((half_pairs, LANES), f32)] * 2
    hbm = pl.BlockSpec(memory_space=pl.ANY)
    steps = n // 2
    staged = pl.pallas_call(
        functools.partial(fused_kernel, count, dims),
        out_shape=[jax.ShapeDtypeStruct(values.shape, bf16)] * 2,
        in_specs=[SM] * 2 + [VM] * 5 + [hbm] * 5,
        out_specs=[hbm] * 2,
        scratch_shapes=[
            pltpu.VMEM((tokens, hidden.shape[1]), bf16),
            pltpu.VMEM((n, 4, packed, gw), bf16), pltpu.VMEM((n, 4, wrows, gw), bf16),
            pltpu.VMEM((packed, gw), bf16), pltpu.VMEM((wrows, gw), bf16),
            pltpu.VMEM((tokens, width), bf16), pltpu.VMEM((tokens, width), bf16),
            *[pltpu.VMEM((tokens, gw), bf16)] * 4,
            pltpu.VMEM((tokens, 2 * gw + 2 * LANES), f32),
            pltpu.VMEM((tokens, heads), f32), pltpu.VMEM((tokens, heads), f32),
            pltpu.VMEM((1, heads), f32), pltpu.VMEM((1, heads), f32),
            *work, *work, *kept, *kept, *box * 9, *gain * 2, *half_gain * 2,
            dma((9,)), dma((2, steps, 4)), dma((2, steps, 4)), dma((n, 4)), dma((n, 4)),
            dma((2,)), dma((2,)), dma((2, half_pairs)), dma((2, half_pairs)), dma((4,)), dma((4,)),
            dma((2, half_pairs)), dma((2, half_pairs)), dma((2, half_pairs)), dma((2, half_pairs)),
            dma((2, half_pairs)), dma((2, half_pairs)), dma((2, npair // BATCH)),
        ],
        compiler_params=pltpu.CompilerParams(
            collective_id=2, has_side_effects=True, vmem_limit_bytes=67_043_328),
        name="fused",
    )(seg_next, seg_prev, dt_bias[None], decay_rate[None], skip_gain[None], proj_dt, dt_prev.T,
      hidden, values, proj_bc, bc_prev, grad)
    chunk = pltpu.VMEM((tokens, width), bf16)
    return pl.pallas_call(
        hand_over,
        out_shape=[jax.ShapeDtypeStruct(values.shape, bf16)] * 2,
        in_specs=[hbm] * 2,
        out_specs=[hbm] * 2,
        scratch_shapes=[chunk, chunk, dma((2, HAND_PARTS)), dma((2, HAND_PARTS))],
        name="hand_over",
    )(*staged)


HAND_PARTS = 8


def hand_over(a_in, b_in, a_out, b_out, a_buf, b_buf, in_sem, out_sem):
    part = a_in.shape[0] // HAND_PARTS
    reads, writes = [], []
    for p in range(HAND_PARTS):
        rows = pl.ds(p * part, part)
        for k, (src, buf, dst) in enumerate(((a_in, a_buf, a_out), (b_in, b_buf, b_out))):
            reads.append(pltpu.make_async_copy(src.at[rows, :], buf.at[rows, :], in_sem.at[k, p]))
            writes.append(pltpu.make_async_copy(buf.at[rows, :], dst.at[rows, :], out_sem.at[k, p]))
    for copy in reads:
        copy.start()
    for read, write in zip(reads, writes):
        read.wait()
        write.start()
    for copy in writes:
        copy.wait()


def body(
    hidden_next, values_next, seg_next, proj_bc, proj_dt, dt_bias, decay_rate, skip_gain,
    bc_prev, dt_prev, seg_prev, grad_prev,
):
    tokens_dev = hidden_next.shape[0]
    bc_width = proj_bc.shape[1]
    heads_all = proj_dt.shape[1]
    fsdp_count = lax.axis_size("fsdp")
    fsdp_place = lax.axis_index("fsdp")
    seq_count = lax.axis_size("seq")
    heads_dev = heads_all // fsdp_count
    state_dim = bc_width // (2 * GW)
    per_group = heads_all // GW
    groups_dev = max(1, heads_dev // per_group)
    first_head = fsdp_place * heads_dev
    first_group = first_head // per_group
    rows_dev = proj_bc.shape[0]
    half = bc_width // 2
    gw = groups_dev * state_dim

    if fsdp_count == 2 and seq_count % 4 == 0 and seq_count >= 8 and heads_all == LANES \
            and rows_dev == 2 * LANES and groups_dev * per_group == heads_dev:
        return fused(hidden_next, values_next, seg_next, proj_bc, proj_dt, dt_bias, decay_rate,
                     skip_gain, bc_prev, dt_prev, seg_prev, grad_prev, gw)

    blocks = []
    for f in range(fsdp_count):
        g0 = (f * heads_dev // per_group) * state_dim
        blocks.append([proj_bc[:, g0:g0 + gw], proj_bc[:, half + g0:half + g0 + gw]])
    ring = fsdp_count == 2 and seq_count % 4 == 0 and rows_dev % (2 * LANES) == 0 and heads_all == LANES
    if ring:
        shard = jnp.concatenate([*blocks[0], *blocks[1], proj_dt], axis=1)
        bc_next, dt_sum = gathered_sums(hidden_next, shard, 2 * gw)
        dt_sum = lax.dynamic_slice_in_dim(dt_sum, first_head, heads_dev, 1)
    else:
        pieces = []
        for f in range(fsdp_count):
            pieces += [*blocks[f], proj_dt[:, f * heads_dev:(f + 1) * heads_dev]]
        weights = lax.all_gather(jnp.concatenate(pieces, axis=1), "seq", axis=0, tiled=True)
        owned = lax.dynamic_slice_in_dim(
            hidden_next.reshape(tokens_dev, seq_count, fsdp_count, rows_dev), fsdp_place, 1, 2
        ).reshape(tokens_dev, seq_count * rows_dev)
        sums = lax.psum_scatter(jnp.dot(owned, weights, preferred_element_type=jnp.float32),
                                "fsdp", scatter_dimension=1, tiled=True)
        bc_next, dt_sum = sums[:, :2 * gw].astype(jnp.bfloat16), sums[:, 2 * gw:]

    decay = lax.dynamic_slice_in_dim(decay_rate, first_head, heads_dev, 0)[None]
    skip = lax.dynamic_slice_in_dim(skip_gain, first_head, heads_dev, 0)[None]
    bias = lax.dynamic_slice_in_dim(dt_bias, first_head, heads_dev, 0)[None]

    b_prev = lax.dynamic_slice_in_dim(bc_prev, first_group * state_dim, gw, 1)
    c_prev = lax.dynamic_slice_in_dim(bc_prev, half + first_group * state_dim, gw, 1)
    b_next, c_next = bc_next[:, :gw], bc_next[:, gw:]
    dt_next = jax.nn.softplus(dt_sum + bias)
    out_next, grad_values = chains(
        seg_next, values_next, c_next, b_next, dt_next, decay, skip,
        seg_prev, grad_prev, b_prev, c_prev, dt_prev)
    return (out_next, grad_values)


def solution(mesh):
    in_specs = (
        P("seq", None), P("seq", "fsdp"), P(), P(("seq", "fsdp"), None), P(("seq", "fsdp"), None),
        P(), P(), P(), P("seq", None), P("seq", "fsdp"), P(), P("seq", "fsdp"),
    )
    out_specs = (P("seq", "fsdp"), P("seq", "fsdp"))
    return jax.shard_map(body, mesh=mesh, in_specs=in_specs, out_specs=out_specs, check_vma=False)
```

```python
import functools

import jax
import jax.numpy as jnp
from jax import lax
from jax.experimental import pallas as pl
from jax.experimental.pallas import tpu as pltpu
from jax.sharding import PartitionSpec as P

GW = 4
SPAN = 128
LANES = 128
MESH = pl.DeviceIdType.MESH


def widen(a, c, head_dim):
    per = LANES // head_dim
    lane = lax.broadcasted_iota(jnp.int32, (1, LANES), 1)
    res = a[:, c * per:c * per + 1]
    for k in range(1, per):
        res = jnp.where(lane >= k * head_dim, a[:, c * per + k:c * per + k + 1], res)
    return jnp.broadcast_to(res, (a.shape[0], LANES))


def seg_maker(len_ref):
    bound = []
    total = jnp.int32(0)
    for k in range(len_ref.shape[0] - 1):
        total = total + len_ref[k]
        bound.append(total)

    def seg_of(pos):
        s = jnp.zeros_like(pos)
        for b in bound:
            s = s + (b <= pos).astype(jnp.int32)
        return s

    return seg_of


def local_states(back, dims, len_ref, x_ref, q_ref, dt_ref, decay_ref, work, pre, keep, part=None):
    nblocks, heads, groups, head_dim = dims
    cum_s, cum_t, dt_t, fout_s = work
    npair = heads * head_dim // LANES
    pair_group = npair // groups
    seg_of = seg_maker(len_ref)
    slab = lax.axis_index("seq") * (nblocks * SPAN)
    dim0 = lax.broadcasted_iota(jnp.int32, (SPAN, SPAN), 0)
    dim1 = lax.broadcasted_iota(jnp.int32, (SPAN, SPAN), 1)
    tril = (dim0 >= dim1).astype(jnp.float32)
    steps = range(nblocks) if part is None else part
    for c in range(npair if 0 in steps else 0):
        pre[0, c] = jnp.zeros((LANES, LANES), jnp.float32)
        keep[0, c] = jnp.ones((1, LANES), jnp.float32)
    for step in steps:
        b = nblocks - 1 - step if back else step
        rows = slice(b * SPAN, (b + 1) * SPAN)
        dt = dt_ref[rows, :]
        cum = jnp.dot(tril, -(dt * decay_ref[...]), precision=lax.Precision.HIGHEST,
                      preferred_element_type=jnp.float32)
        end = cum[SPAN - 1:SPAN, :]
        cum_s[rows, :] = cum
        cum_t[b] = cum.T
        dt_t[b] = dt.T
        seg = seg_of(slab + b * SPAN + lax.broadcasted_iota(jnp.int32, (SPAN, heads), 0))
        edge = slab + b * SPAN + lax.broadcasted_iota(jnp.int32, (1, heads), 0) * 0
        seg_e = seg_of(edge + (SPAN - 1))
        seg_b = jnp.where(edge == 0, 0, seg_of(edge - 1))
        send = jnp.where(seg == seg_e, jnp.exp(end - cum), 0.0) * dt
        read = jnp.where(seg == seg_b, jnp.exp(cum), 0.0)
        carry = jnp.where(seg_e == seg_b, jnp.exp(end), 0.0)
        f_in = read if back else send
        fout_s[rows, :] = send if back else read
        qt = [q_ref[rows, g * LANES:(g + 1) * LANES].T for g in range(groups)]
        for c in range(npair):
            cols = slice(c * LANES, (c + 1) * LANES)
            sent = (x_ref[rows, cols].astype(jnp.float32) * widen(f_in, c, head_dim)).astype(jnp.bfloat16)
            loc = jnp.dot(qt[c // pair_group], sent, preferred_element_type=jnp.float32)
            wide = widen(carry, c, head_dim)
            pre[step + 1, c] = wide * pre[step, c] + loc
            keep[step + 1, c] = wide * keep[step, c]


def in_block(back, dims, len_ref, x_ref, p_ref, q_ref, dt_ref, skip_ref, work, inside, fexp, span=None,
             only=None):
    nblocks, heads, groups, head_dim = dims
    cum_s, cum_t, dt_t, fout_s = work
    npair = heads * head_dim // LANES
    per = LANES // head_dim
    pair_group = npair // groups
    seg_of = seg_maker(len_ref)
    slab = lax.axis_index("seq") * (nblocks * SPAN)
    dim0 = lax.broadcasted_iota(jnp.int32, (SPAN, SPAN), 0)
    dim1 = lax.broadcasted_iota(jnp.int32, (SPAN, SPAN), 1)
    lane = lax.broadcasted_iota(jnp.int32, (1, LANES), 1)

    def one(b, _):
        start = pl.multiple_of(b * SPAN, SPAN)
        rows = pl.ds(start, SPAN)
        seg_i = seg_of(slab + start + dim0)
        seg_j = seg_of(slab + start + dim1)
        order = (dim1 >= dim0) if back else (dim1 <= dim0)
        bias = jnp.where((seg_i == seg_j) & order, 0.0, -jnp.inf)
        cum = cum_s[rows, :]
        dt = dt_ref[rows, :]
        f_out = fout_s[rows, :]
        for g in range(groups) if only is None else (only,):
            gl = slice(g * LANES, (g + 1) * LANES)
            score = lax.dot_general(p_ref[rows, gl], q_ref[rows, gl], (((1,), (1,)), ((), ())),
                                    preferred_element_type=jnp.float32)
            for c in range(g * pair_group, (g + 1) * pair_group):
                cols = slice(c * LANES, (c + 1) * LANES)
                x = x_ref[rows, cols]
                mixes, parts = [], []
                for k in range(per):
                    h = c * per + k
                    col = cum[:, h:h + 1]
                    row = cum_t[b, h:h + 1, :]
                    spread = (row - col) if back else (col - row)
                    w = jnp.exp(spread + bias) * score
                    if not back:
                        w = w * dt_t[b, h:h + 1, :]
                    mixes.append(w.astype(jnp.bfloat16))
                    mine = (lane >= k * head_dim) & (lane < (k + 1) * head_dim)
                    parts.append(jnp.where(mine, x, jnp.zeros_like(x)))
                acc = jnp.dot(jnp.concatenate(mixes, 1), jnp.concatenate(parts, 0),
                              preferred_element_type=jnp.float32)
                if back:
                    acc = acc * widen(dt, c, head_dim)
                inside[c, rows, :] = acc + widen(skip_ref[...], c, head_dim) * x.astype(jnp.float32)
                fexp[c, rows, :] = widen(f_out, c, head_dim)
        return 0

    first, last = (0, nblocks) if span is None else span
    lax.fori_loop(first, last, one, 0)


HOP_CHUNKS = 5


def chain_kernel(count, dims, len_ref, x_ref, p_ref, q_ref, dt_ref, decay_ref, skip_ref,
                 lenb_ref, xb_ref, pb_ref, qb_ref, dtb_ref,
                 out_ref, grad_ref, *scratch):
    work, work_b, rest = scratch[:4], scratch[4:8], scratch[12:]
    inside_b, fexp_b, pre_b, keep_b = scratch[8:12]
    inside, fexp, pre, keep, inbox, outbox, in_b, out_b, s_sem, r_sem, sb_sem, rb_sem = rest
    nblocks, heads, groups, head_dim = dims
    npair = heads * head_dim // LANES
    pair_group = npair // groups
    me = lax.axis_index("seq")
    low, high = me == 0, me == count - 1

    barrier = pltpu.get_barrier_semaphore()

    @pl.when(jnp.logical_not(low))
    def _():
        pl.semaphore_signal(barrier, inc=1, device_id={"seq": me - 1}, device_id_type=MESH)

    @pl.when(jnp.logical_not(high))
    def _():
        pl.semaphore_signal(barrier, inc=1, device_id={"seq": me + 1}, device_id_type=MESH)

    local_states(False, dims, len_ref, x_ref, q_ref, dt_ref, decay_ref, work, pre, keep)
    local_states(True, dims, lenb_ref, xb_ref, qb_ref, dtb_ref, decay_ref, work_b, pre_b, keep_b)

    @pl.when(low)
    def _():
        inbox[...] = jnp.zeros_like(inbox)

    @pl.when(high)
    def _():
        in_b[...] = jnp.zeros_like(in_b)

    pl.semaphore_wait(barrier, jnp.where(low, 0, 1) + jnp.where(high, 0, 1))

    def hop(back, c):
        return pltpu.make_async_remote_copy(
            src_ref=(out_b if back else outbox).at[c], dst_ref=(in_b if back else inbox).at[c],
            send_sem=(sb_sem if back else s_sem).at[c], recv_sem=(rb_sem if back else r_sem).at[c],
            device_id={"seq": me - 1 if back else me + 1}, device_id_type=MESH)

    def relay(back, c):
        first, last = (high, low) if back else (low, high)
        kp, pr = (keep_b, pre_b) if back else (keep, pre)

        @pl.when(jnp.logical_not(first))
        def _():
            hop(back, c).wait_recv()

        @pl.when(jnp.logical_not(last))
        def _():
            state = (in_b if back else inbox)[c].astype(jnp.float32)
            (out_b if back else outbox)[c] = (kp[nblocks, c] * state + pr[nblocks, c]).astype(jnp.bfloat16)
            hop(back, c).start()

    def finish(back, c):
        kp, pr, ins, fx, vec, out = (
            (keep_b, pre_b, inside_b, fexp_b, pb_ref, grad_ref) if back
            else (keep, pre, inside, fexp, p_ref, out_ref))
        g = c // pair_group
        cols = pl.ds(pl.multiple_of(c * LANES, LANES), LANES)
        gl = pl.ds(pl.multiple_of(g * LANES, LANES), LANES)
        state = (in_b if back else inbox)[c].astype(jnp.float32)
        for step in range(nblocks):
            b = nblocks - 1 - step if back else step
            rows = slice(b * SPAN, (b + 1) * SPAN)
            entering = (kp[step, c] * state + pr[step, c]).astype(jnp.bfloat16)
            y = jnp.dot(vec[rows, gl], entering, preferred_element_type=jnp.float32)
            out[rows, cols] = (ins[c, rows, :] + fx[c, rows, :] * y).astype(jnp.bfloat16)

    lag = (2 * me - (count - 1)) * HOP_CHUNKS
    up_first = lag < 0
    gap = jnp.where(up_first, -lag, lag)
    block_at = jnp.where(gap >= npair, npair, 0)

    def step_of(i, _):
        @pl.when(i == block_at)
        def _():
            in_block(False, dims, len_ref, x_ref, p_ref, q_ref, dt_ref, skip_ref, work, inside, fexp)
            in_block(True, dims, lenb_ref, xb_ref, pb_ref, qb_ref, dtb_ref, skip_ref, work_b, inside_b, fexp_b)

        for back in (False, True):
            leads = jnp.logical_not(up_first) if back else up_first
            c = i - jnp.where(leads, 0, gap)

            @pl.when((c >= 0) & (c < npair))
            def _(back=back, c=c):
                relay(back, c)

            done = jnp.where(leads, i - npair, c)

            @pl.when((done >= 0) & (done < npair))
            def _(back=back, done=done):
                finish(back, done)

        return 0

    lax.fori_loop(0, npair + jnp.maximum(gap, npair), step_of, 0)

    def drain(c, _):
        @pl.when(jnp.logical_not(high))
        def _():
            hop(False, c).wait_send()

        @pl.when(jnp.logical_not(low))
        def _():
            hop(True, c).wait_send()

        return 0

    lax.fori_loop(0, npair, drain, 0)


def sizes_of(x, p_vec, dt):
    tokens, width = x.shape
    heads = dt.shape[1]
    dims = (tokens // SPAN, heads, p_vec.shape[1] // LANES, width // heads)
    nblocks, npair = dims[0], width // LANES
    f32 = jnp.float32
    work = [pltpu.VMEM((tokens, heads), f32), pltpu.VMEM((nblocks, heads, SPAN), f32),
            pltpu.VMEM((nblocks, heads, SPAN), f32), pltpu.VMEM((tokens, heads), f32)]
    kept = [(npair, tokens, LANES), (npair, tokens, LANES),
            (nblocks + 1, npair, LANES, LANES), (nblocks + 1, npair, 1, LANES)]
    return dims, npair, work, kept


VM = pl.BlockSpec(memory_space=pltpu.VMEM)
SM = pl.BlockSpec(memory_space=pltpu.SMEM)


def chains(lengths, x, p_vec, q_vec, dt, decay, skip, *back):
    dims, npair, work, kept = sizes_of(x, p_vec, dt)
    box = pltpu.VMEM((npair, LANES, LANES), jnp.bfloat16)
    sem = pltpu.SemaphoreType.DMA((npair,))
    return pl.pallas_call(
        functools.partial(chain_kernel, lax.axis_size("seq"), dims),
        out_shape=[jax.ShapeDtypeStruct(x.shape, jnp.bfloat16)] * 2,
        in_specs=[SM] + [VM] * 6 + [SM] + [VM] * 4,
        out_specs=[VM] * 2,
        scratch_shapes=(work * 2 + [pltpu.VMEM(k, jnp.float32) for k in kept] * 2
                        + [box] * 4 + [sem] * 4),
        compiler_params=pltpu.CompilerParams(
            collective_id=0, has_side_effects=True, vmem_limit_bytes=56 * 1024 * 1024),
        cost_estimate=pl.CostEstimate(flops=40_000_000_000, bytes_accessed=40_000_000, transcendentals=0),
        name="chains",
    )(lengths, x, p_vec, q_vec, dt, decay, skip, *back)


PIECES = 4


def gather_kernel(count, h_ref, w_ref, bc_ref, dt_ref,
                  held, acc, bc_out, bc_in, dt_out, dt_in,
                  ring_s, ring_r, side_s, side_r, x_s, x_r):
    me, f = lax.axis_index("seq"), lax.axis_index("fsdp")
    n = count // 2
    half_ring = n // 2
    core, chip = me % 2, me // 2
    r = jnp.where(chip % 2 == 0, chip // 2, n - 1 - chip // 2)
    rows = w_ref.shape[0]
    piece = rows // PIECES
    wide = bc_ref.shape[1]

    def id_of(pos, which):
        p = (pos + 2 * n) % n
        up = p < half_ring
        return jnp.where(up, p * 2, (n - 1 - p) * 2 + 1) * 2 + which

    nxt, prv, partner = id_of(r + 1, core), id_of(r - 1, core), chip * 2 + 1 - core

    barrier = pltpu.get_barrier_semaphore()
    for peer in (nxt, prv, partner):
        pl.semaphore_signal(barrier, inc=1, device_id={"seq": peer}, device_id_type=MESH)
    pl.semaphore_signal(barrier, inc=1, device_id={"fsdp": 1 - f}, device_id_type=MESH)
    pl.semaphore_wait(barrier, 4)

    def part(p):
        return pl.ds(p * piece, piece)

    def origin(step, p, which):
        return id_of(r - step if p < PIECES // 2 else r + step, which)

    def ring_copy(step, p, src):
        return pltpu.make_async_remote_copy(
            src_ref=src, dst_ref=held.at[origin(step, p, core), part(p), :],
            send_sem=ring_s.at[step, p], recv_sem=ring_r.at[step, p],
            device_id={"seq": nxt if p < PIECES // 2 else prv}, device_id_type=MESH)

    def side_copy(step, p, src):
        return pltpu.make_async_remote_copy(
            src_ref=src, dst_ref=held.at[origin(step, p, core), part(p), :],
            send_sem=side_s.at[step, p], recv_sem=side_r.at[step, p],
            device_id={"seq": partner}, device_id_type=MESH)

    def landed(step, p):
        return held.at[origin(step, p, core), part(p), :]

    for p in range(PIECES):
        ring_copy(0, p, w_ref.at[part(p), :]).start()
    for p in range(PIECES):
        side_copy(0, p, w_ref.at[part(p), :]).start()

    def columns(seq_index, first):
        start = (seq_index * 2 + f) * rows + first
        return h_ref[:, pl.ds(pl.multiple_of(start, rows // 2), rows // 2)]

    def mac(step, which):
        half = rows // 2
        lo, hi = origin(step, 0, which), origin(step, PIECES - 1, which)
        left = jnp.concatenate([columns(lo, 0), columns(hi, half)], axis=1)
        right = jnp.concatenate([held[lo, 0:half, :], held[hi, half:, :]], axis=0)
        acc[...] += jnp.dot(left, right, preferred_element_type=jnp.float32)

    acc[...] = jnp.dot(jnp.concatenate([columns(me, 0), columns(me, rows // 2)], axis=1), w_ref[...],
                       preferred_element_type=jnp.float32)

    def one(step, _):
        for p in (0, PIECES // 2, 1, PIECES // 2 + 1):
            ring_copy(step, p, landed(step, p)).wait_recv()

            @pl.when(step < n - 2)
            def _(p=p):
                ring_copy(step + 1, p, landed(step + 1, p)).start()

            side_copy(step + 1, p, landed(step + 1, p)).start()
        mac(step + 1, core)
        for p in range(PIECES):
            side_copy(step, p, landed(step, p)).wait_recv()
        mac(step, 1 - core)
        return 0

    lax.fori_loop(0, n - 1, one, 0)
    for p in range(PIECES):
        side_copy(n - 1, p, landed(n - 1, p)).wait_recv()
    mac(n - 1, 1 - core)

    def cross(src, dst, k):
        return pltpu.make_async_remote_copy(
            src_ref=src, dst_ref=dst, send_sem=x_s.at[k], recv_sem=x_r.at[k],
            device_id={"fsdp": 1 - f}, device_id_type=MESH)

    def side_of(which):
        return pl.ds(pl.multiple_of(which * wide, wide), wide)

    bc_out[...] = acc[:, side_of(1 - f)]
    dt_out[...] = acc[:, 2 * wide:]
    cross(bc_out, bc_in, 0).start()
    cross(dt_out, dt_in, 1).start()

    def drain(step, _):
        for p in range(PIECES):
            @pl.when(step < n - 1)
            def _(p=p):
                ring_copy(step, p, landed(step, p)).wait_send()

            side_copy(step, p, landed(step, p)).wait_send()
        return 0

    lax.fori_loop(0, n, drain, 0)
    cross(bc_out, bc_in, 0).wait()
    bc_ref[...] = (acc[:, side_of(f)] + bc_in[...]).astype(jnp.bfloat16)
    cross(dt_out, dt_in, 1).wait()
    dt_ref[...] = acc[:, 2 * wide:] + dt_in[...]


def gathered_sums(hidden, shard, wide):
    count = lax.axis_size("seq")
    tokens, total = hidden.shape[0], shard.shape[1]
    f32, bf16 = jnp.float32, jnp.bfloat16
    n = count // 2
    dma = pltpu.SemaphoreType.DMA
    return pl.pallas_call(
        functools.partial(gather_kernel, count),
        out_shape=[jax.ShapeDtypeStruct((tokens, wide), bf16),
                   jax.ShapeDtypeStruct((tokens, total - 2 * wide), f32)],
        in_specs=[VM] * 2,
        out_specs=[VM] * 2,
        scratch_shapes=[
            pltpu.VMEM((count,) + shard.shape, bf16),
            pltpu.VMEM((tokens, total), f32),
            pltpu.VMEM((tokens, wide), f32), pltpu.VMEM((tokens, wide), f32),
            pltpu.VMEM((tokens, total - 2 * wide), f32), pltpu.VMEM((tokens, total - 2 * wide), f32),
            dma((n, PIECES)), dma((n, PIECES)), dma((n, PIECES)), dma((n, PIECES)), dma((2,)), dma((2,)),
        ],
        compiler_params=pltpu.CompilerParams(
            collective_id=1, has_side_effects=True, vmem_limit_bytes=32 * 1024 * 1024),
        cost_estimate=pl.CostEstimate(flops=40_000_000_000, bytes_accessed=40_000_000, transcendentals=0),
        name="gather_project",
    )(hidden, shard)


Z_LAG = 6
BLOCK_GAP = 3
CORE_LAG = 3
BATCH = 4
EARLY = 4


def fused_kernel(count, dims, len_ref, lenb_ref, bias_in, decay_in, skip_in, pdt_ref, dtt_ref,
                 h_hbm, x_hbm, w_hbm, bcp_hbm, g_hbm, out_hbm, grad_hbm,
                 hid, held_b, held_c, yout_b, yout_c, xv, gv, bp, cp, bn, cn, acc, dtn, dtp, decay_ref, skip_ref,
                 *scratch):
    work, work_b = scratch[:4], scratch[4:8]
    kept = (scratch[8:12], scratch[12:16])
    lout, lin, xout, xin, zout, zin, eout, ein, eown, kv, ksib, kxo, kxi = (
        (scratch[16 + 2 * i], scratch[17 + 2 * i]) for i in range(13))
    (ld, ring_s, ring_r, side_s, side_r, y_s, y_r, l_s, l_r, k_s, k_r, c_s, c_r, z_s, z_r,
     e_s, e_r, o_sem) = scratch[42:]
    nblocks, heads, groups, head_dim = dims
    npair = heads * head_dim // LANES
    pair_group = npair // groups
    half_pairs = npair // 2
    me, f = lax.axis_index("seq"), lax.axis_index("fsdp")
    core, chip = me % 2, me // 2
    xpos, zpos, nz = chip % 2, chip // 2, count // 4
    n = count // 2
    half_ring = n // 2
    full = half_ring - 1
    far = 2 * full + 1
    gw = groups * LANES
    wrows = w_hbm.shape[0]
    r = jnp.where(xpos == 0, zpos, n - 1 - zpos)

    def chip_at(pos):
        p = (pos + 2 * n) % n
        return jnp.where(p < half_ring, p * 2, (n - 1 - p) * 2 + 1)

    nxt, prv = chip_at(r + 1) * 2 + core, chip_at(r - 1) * 2 + core
    partner = chip * 2 + 1 - core
    xpeer = (zpos * 2 + 1 - xpos) * 2 + core
    own, other = core * 2 + f, core * 2 + 1 - f

    def at_cols(start):
        return pl.ds(pl.multiple_of(start, LANES), gw)

    def load(src, dst, k):
        return pltpu.make_async_copy(src, dst, ld.at[k])

    w_half = w_hbm.shape[1] // 2
    w_loads = [
        load(w_hbm.at[:, at_cols(f * gw)], held_b.at[chip, own, 0:wrows, :], 0),
        load(w_hbm.at[:, at_cols((1 - f) * gw)], yout_b.at[0:wrows, :], 1),
        load(w_hbm.at[:, at_cols(w_half + f * gw)], held_c.at[chip, own, :, :], 2),
        load(w_hbm.at[:, at_cols(w_half + (1 - f) * gw)], yout_c, 3),
    ]
    b_loads = [
        load(g_hbm, gv, 4),
        load(bcp_hbm.at[:, at_cols(f * gw)], bp, 5),
        load(bcp_hbm.at[:, at_cols(w_half + f * gw)], cp, 6),
    ]
    h_load, x_load = load(h_hbm, hid, 7), load(x_hbm, xv, 8)
    for copy in (*w_loads, *b_loads, h_load, x_load):
        copy.start()

    barrier = pltpu.get_barrier_semaphore()
    for peer in (partner, xpeer):
        pl.semaphore_signal(barrier, inc=1, device_id={"seq": peer}, device_id_type=MESH)
    pl.semaphore_signal(barrier, inc=1, device_id={"fsdp": 1 - f}, device_id_type=MESH)

    @pl.when(zpos > 0)
    def _():
        pl.semaphore_signal(barrier, inc=1, device_id={"seq": me - 4}, device_id_type=MESH)

    @pl.when(zpos < nz - 1)
    def _():
        pl.semaphore_signal(barrier, inc=1, device_id={"seq": me + 4}, device_id_type=MESH)

    lane = lax.broadcasted_iota(jnp.int32, (LANES, LANES), 1)
    top = pdt_ref[0:LANES, :].astype(jnp.float32)
    low = pdt_ref[LANES:2 * LANES, :].astype(jnp.float32)
    pack0 = jnp.where(lane < heads, top, pltpu.roll(low, heads, 1))
    pack1 = jnp.where(lane < heads, pltpu.roll(top, heads, 1), low)
    mine = jnp.where(f == 0, pack0, pack1).astype(jnp.bfloat16)
    theirs = jnp.where(f == 0, pack1, pack0).astype(jnp.bfloat16)
    strips = gw // LANES
    strip = LANES // strips
    for k in range(strips):
        lanes = slice(k * LANES, (k + 1) * LANES)
        held_b[chip, own, wrows:wrows + strip, lanes] = mine[k * strip:(k + 1) * strip, :]
        yout_b[wrows:wrows + strip, lanes] = theirs[k * strip:(k + 1) * strip, :]
    decay_ref[...] = jnp.where(f == 0, decay_in[:, 0:heads], decay_in[:, heads:2 * heads])
    skip_ref[...] = jnp.where(f == 0, skip_in[:, 0:heads], skip_in[:, heads:2 * heads])
    bias = jnp.where(f == 0, bias_in[:, 0:heads], bias_in[:, heads:2 * heads])
    for b in range(nblocks):
        dtp[b * SPAN:(b + 1) * SPAN, :] = dtt_ref[:, b * SPAN:(b + 1) * SPAN].T

    pl.semaphore_wait(barrier, 3 + jnp.where(zpos > 0, 1, 0) + jnp.where(zpos < nz - 1, 1, 0))
    for copy in w_loads:
        copy.wait()

    def piece(where, j, mine=True):
        base = (core if mine else 1 - core) * 2
        return (held_b if j < 2 else held_c).at[where, base + (f if j % 2 == 0 else 1 - f)]

    def remote(src, dst, s, rv, **peer):
        return pltpu.make_async_remote_copy(src_ref=src, dst_ref=dst, send_sem=s, recv_sem=rv,
                                            device_id=peer, device_id_type=MESH)

    def ring(d, k, j, arrived=False):
        away = k if arrived else k - 1
        ref = piece(chip_at(r - away if d == 0 else r + away), j)
        return remote(ref, ref, ring_s.at[d, k - 1, j // 2], ring_r.at[d, k - 1, j],
                      seq=nxt if d == 0 else prv)

    def chip_of(u):
        return chip_at(r - u if u <= full else (r + (u - full) if u < far else r + half_ring))

    def side(u, j):
        ref = piece(chip_of(u), j)
        return remote(ref, ref, side_s.at[u, j // 2], side_r.at[u, j // 2], seq=partner)

    def both(where, kind, mine=True):
        return (held_c if kind else held_b).at[where, pl.ds((core if mine else 1 - core) * 2, 2)]

    def side_both(u, kind, arrived=False):
        ref = both(chip_of(u), kind, not arrived)
        return remote(ref, ref, side_s.at[u, kind], side_r.at[u, kind], seq=partner)

    def cross(kind, arrived=False):
        ref = held_c if kind else held_b
        return remote(yout_c if kind else yout_b, ref.at[chip, other if arrived else own],
                      y_s.at[kind], y_r.at[kind], fsdp=1 - f)

    def begin(j):
        ring(0, 1, j).start()
        ring(1, 1, j).start()
        side(0, j).start()

    for kind in range(2):
        cross(kind).start()
        begin(2 * kind)

    def receive(k, kind, second=False):
        for d in range(2):
            if k > full and second:
                continue
            j = 2 * kind + ((1 - d if second else d) if k > 1 or kind else int(second))
            ring(d, k, j, True).wait_recv()
            if k < full or (k == full and j % 2 == d):
                ring(d, k + 1, j).start()
            side(far if k > full else (k if d == 0 else full + k), j).start()

    wide = 4 * wrows

    def add(at, value, first):
        cols = slice(at, at + value.shape[1])
        acc[:, cols] = value if first else acc[:, cols] + value

    def mac(u, kind, first=False):
        side_both(u, kind, True).wait_recv()
        q = chip_of(u)
        left = hid[:, pl.ds(pl.multiple_of(q * wide, wide), wide)]
        ref = held_c if kind else held_b
        add(gw + 2 * LANES if kind else 0,
            jnp.dot(left, jnp.concatenate([ref[q, s, 0:wrows, :] for s in range(4)], axis=0),
                    preferred_element_type=jnp.float32), first)
        if kind == 0:
            packs = jnp.concatenate(
                [held_b[q, s, wrows:wrows + strip, k * LANES:(k + 1) * LANES]
                 for s in range(4) for k in range(strips)], axis=0)
            for o in range(2):
                part = jnp.concatenate(
                    [left[:, s * wrows + o * LANES:s * wrows + (o + 1) * LANES] for s in range(4)], axis=1)
                add(gw + o * LANES, jnp.dot(part, packs, preferred_element_type=jnp.float32), first)

    def l_copy(back):
        return remote(lout[back], lin[back], l_s.at[back], l_r.at[back], seq=partner)

    def exchange(back):
        pre, keep = kept[back][2:]
        for c in range(npair):
            kv[back][c:c + 1, :] = keep[nblocks, c]
        remote(kv[back], ksib[back], k_s.at[back], k_r.at[back], seq=partner).start()

        def put(i, _):
            lout[back][i] = pre[nblocks, (1 - core) * half_pairs + i].astype(jnp.bfloat16)
            return 0

        lax.fori_loop(0, half_pairs, put, 0)
        l_copy(back).start()

    def lead_core(back):
        return (core == 1) if back else (core == 0)

    def lead_x(back):
        return (xpos == 1) if back else (xpos == 0)

    def ends(back):
        return (zpos == 0) if back else (zpos == nz - 1)

    def gives(back):
        return jnp.logical_not(ends(back)) | lead_x(back)

    def takes(back):
        return jnp.logical_not(ends(back) & lead_x(back))

    def row(ref, i):
        return ref[pl.ds(i, 1), :]

    def x_copy(back, i):
        return remote(xout[back].at[i], xin[back].at[i], c_s.at[back], c_r.at[back, i], seq=xpeer)

    def kx_copy(back):
        return remote(kxo[back], kxi[back], k_s.at[2 + back], k_r.at[2 + back], seq=xpeer)

    def combine(back):
        rows = pl.ds(pl.multiple_of(core * half_pairs, half_pairs), half_pairs)
        remote(kv[back], ksib[back], k_s.at[back], k_r.at[back], seq=partner).wait_recv()
        kxo[back][...] = kv[back][rows, :] * ksib[back][rows, :]
        sends = gives(back)

        @pl.when(sends)
        def _():
            kx_copy(back).start()

    def combine_part(back, send):
        l_copy(back).wait_recv()
        pre = kept[back][2]
        sends = gives(back)

        def put(i, _):
            g = core * half_pairs + i
            lead = lead_core(back)
            total = (pre[nblocks, g] * jnp.where(lead, row(ksib[back], g), 1.0)
                     + lin[back][i].astype(jnp.float32) * jnp.where(lead, 1.0, row(kv[back], g)))
            xout[back][i] = total.astype(jnp.bfloat16)
            if send:
                @pl.when(sends)
                def _():
                    x_copy(back, i).start()

            return 0

        lax.fori_loop(0, half_pairs, put, 0)

    def x_sends(back, start, stop):
        def put(i, _):
            x_copy(back, i).start()
            return 0

        @pl.when(gives(back))
        def _():
            lax.fori_loop(start, stop, put, 0)

    def z_copy(back, i):
        return remote(zout[back].at[i], zin[back].at[i], z_s.at[back], z_r.at[back, i],
                      seq=me - 4 if back else me + 4)

    def e_copy(back, k):
        part = pl.ds(k * BATCH, BATCH)
        return remote(eout[back].at[part], ein[back].at[part], e_s.at[back], e_r.at[back, k], seq=partner)

    def out_copy(back, k):
        cols = pl.ds(pl.multiple_of(k * BATCH * LANES, LANES), BATCH * LANES)
        src, dst = (gv, grad_hbm) if back else (xv, out_hbm)
        return pltpu.make_async_copy(src.at[:, cols], dst.at[:, cols], o_sem.at[back])

    def finish(back, c0, states, i0):
        ins, fx, pre, keep = kept[back]
        vec, out = (bp, gv) if back else (cn, xv)
        gl = pl.ds(pl.multiple_of((c0 // pair_group) * LANES, LANES), LANES)
        for step in range(nblocks):
            b = nblocks - 1 - step if back else step
            rows = slice(b * SPAN, (b + 1) * SPAN)
            for k in range(0, BATCH, 2):
                entering = []
                for c, i in ((c0 + k, i0 + k), (c0 + k + 1, i0 + k + 1)):
                    state = states[i]
                    if step > 0:
                        state = (keep[step, c] * state.astype(jnp.float32) + pre[step, c]).astype(jnp.bfloat16)
                    entering.append(state)
                y = jnp.dot(vec[rows, gl], jnp.concatenate(entering, axis=1), preferred_element_type=jnp.float32)
                for m in range(2):
                    c = c0 + k + m
                    cols = pl.ds(pl.multiple_of(c * LANES, LANES), LANES)
                    part = y[:, m * LANES:(m + 1) * LANES]
                    out[rows, cols] = (ins[c, rows, :] + fx[c, rows, :] * part).astype(jnp.bfloat16)
        out_copy(back, c0 // BATCH).start()

    def relay(back, i):
        pre = kept[back][2]
        g = core * half_pairs + i
        z_first, z_last = (zpos == nz - 1, zpos == 0) if back else (zpos == 0, zpos == nz - 1)

        @pl.when((i == 0) & takes(back))
        def _():
            kx_copy(back).wait_recv()

        @pl.when((i == 0) & jnp.logical_not(takes(back)))
        def _():
            kxi[back][...] = jnp.zeros_like(kxi[back])

        @pl.when(takes(back))
        def _():
            x_copy(back, i).wait_recv()

        @pl.when(jnp.logical_not(z_first))
        def _():
            z_copy(back, i).wait_recv()

        k_own, k_peer = row(kxo[back], i), row(kxi[back], i)
        l_own = xout[back][i].astype(jnp.float32)
        l_peer = jnp.where(takes(back), xin[back][i].astype(jnp.float32), 0.0)
        state = jnp.where(z_first, 0.0, zin[back][i].astype(jnp.float32))
        lead = lead_x(back)
        zout[back][i] = (k_own * k_peer * state + l_own * jnp.where(lead, k_peer, 1.0)
                         + l_peer * jnp.where(lead, 1.0, k_own)).astype(jnp.bfloat16)

        @pl.when(jnp.logical_not(z_last))
        def _():
            z_copy(back, i).start()

        state = jnp.where(lead, state, k_peer * state + l_peer)
        head = lead_core(back)
        k_lead = jnp.where(head, row(kv[back], g), row(ksib[back], g))
        l_lead = jnp.where(head, pre[nblocks, g], lin[back][i].astype(jnp.float32))
        after = k_lead * state + l_lead
        eout[back][i] = jnp.where(head, after, state).astype(jnp.bfloat16)

        @pl.when(i % BATCH == BATCH - 1)
        def _():
            e_copy(back, i // BATCH).start()

        eown[back][i] = jnp.where(head, state, after).astype(jnp.bfloat16)

    def settle(back, i):
        e_copy(back, i // BATCH).wait_recv()
        finish(back, core * half_pairs + i, eown[back], i)
        finish(back, (1 - core) * half_pairs + i, ein[back], i)

    def block(back, b):
        if back:
            in_block(True, dims, lenb_ref, gv, bp, cp, dtp, skip_ref, work_b, *kept[1][:2], span=(b, b + 1))
        else:
            at, g = b
            in_block(False, dims, len_ref, xv, cn, bn, dtn, skip_ref, work, *kept[0][:2],
                     span=(at, at + 1), only=g)

    for copy in b_loads:
        copy.wait()
    local_states(True, dims, lenb_ref, gv, cp, dtp, decay_ref, work_b, *kept[1][2:])
    for kind in range(2):
        cross(kind, True).wait_recv()
        begin(2 * kind + 1)
    receive(1, 0)
    exchange(1)
    block(True, 0)
    receive(1, 0, True)
    receive(1, 1)
    block(True, 1)
    combine(1)
    combine_part(1, False)
    outer = (zpos == 0) | (zpos == nz - 1)
    x_sends(1, 0, jnp.where(outer, 0, half_pairs))
    h_load.wait()
    mac(0, 0, True)
    c_next = [(k, second) for k in range(1, full + 1) for second in (False, True)][1:]
    for k in range(2, full + 1):
        receive(k, 0)
        receive(k, 0, True)
        if k == 2:
            mac(0, 1, True)
        for u in (k - 1, full + k - 1):
            mac(u, 0)
        for _ in range(2 if k == full else 1):
            step, second = c_next.pop(0)
            receive(step, 1, second)
        if k == 2:
            for u in (1, full + 1):
                mac(u, 1)
    for u in (full, 2 * full):
        mac(u, 0)
    receive(full + 1, 0)
    x_load.wait()
    mac(far, 0)
    at = gw
    bn[...] = acc[:, 0:gw].astype(jnp.bfloat16)
    dt_sum = acc[:, at:at + heads] + acc[:, at + LANES + heads:at + LANES + 2 * heads] + bias
    dtn[...] = jnp.maximum(dt_sum, 0.0) + jnp.log1p(jnp.exp(-jnp.abs(dt_sum)))

    def forward_states(steps):
        local_states(False, dims, len_ref, xv, bn, dtn, decay_ref, work, *kept[0][2:], part=steps)

    forward_states((0,))
    while len(c_next) > 1:
        step, second = c_next.pop(0)
        receive(step, 1, second)
    early = jnp.where(zpos == 0, EARLY, half_pairs)
    x_sends(1, jnp.where(outer, 0, half_pairs), early)
    forward_states(range(1, nblocks))
    exchange(0)
    for step, second in c_next:
        receive(step, 1, second)
    for u in (2, full + 2):
        mac(u, 1)
    combine(0)
    combine_part(0, True)
    x_sends(1, early, half_pairs)
    for k in range(3, full + 1):
        for u in (k, full + k):
            mac(u, 1)
    receive(full + 1, 1)
    mac(far, 1)
    cn[...] = acc[:, gw + 2 * LANES:].astype(jnp.bfloat16)
    block_end = 1 + BLOCK_GAP * (groups * nblocks - 1)

    def tick(t, _):
        for back in range(2):
            i = t - ((nz - 1 - zpos) if back else zpos) * Z_LAG

            @pl.when((i >= 0) & (i < half_pairs))
            def _(back=back, i=i):
                relay(back, i)

        for g in range(groups):
            u = (t - 1) // BLOCK_GAP - g * nblocks

            @pl.when(((t - 1) % BLOCK_GAP == 0) & (u >= 0) & (u < nblocks))
            def _(u=u, g=g):
                block(False, (u, g))

        for back in range(2):
            lag = ((nz - 1 - zpos) if back else zpos) * Z_LAG + CORE_LAG
            late = t - (lag if back else jnp.maximum(lag, block_end + 2 - BATCH))

            @pl.when((late >= 0) & (late < half_pairs) & (late % BATCH == BATCH - 1))
            def _(back=back, late=late):
                settle(back, late - (BATCH - 1))

        return 0

    last = max(half_pairs + CORE_LAG + (nz - 1) * Z_LAG, half_pairs + block_end + 2 - BATCH)
    lax.fori_loop(0, last, tick, 0)

    for j in range(2):
        cross(j).wait_send()
    for k in range(1, half_ring + 1):
        for d in range(2):
            for kind in range(2):
                if k > full:
                    ring(d, k, 2 * kind + d).wait_send()
                else:
                    ref = both(chip, kind)
                    remote(ref, ref, ring_s.at[d, k - 1, kind], ring_r.at[d, k - 1, 2 * kind],
                           seq=partner).wait_send()
    for u in range(far + 1):
        for kind in range(2):
            side_both(u, kind).wait_send()
    for back in range(2):
        remote(kv[back], ksib[back], k_s.at[back], k_r.at[back], seq=partner).wait_send()
        given = gives(back)

        @pl.when(given)
        def _(back=back):
            kx_copy(back).wait_send()

        @pl.when(given)
        def _(back=back):
            remote(xout[back], xin[back], c_s.at[back], c_r.at[back, 0], seq=xpeer).wait_send()

        @pl.when(zpos != (0 if back else nz - 1))
        def _(back=back):
            remote(zout[back], zin[back], z_s.at[back], z_r.at[back, 0], seq=xpeer).wait_send()

        l_copy(back).wait_send()
        remote(eout[back], ein[back], e_s.at[back], e_r.at[back, 0], seq=partner).wait_send()
        pltpu.make_async_copy(*((gv, grad_hbm) if back else (xv, out_hbm)), o_sem.at[back]).wait()


def fused(hidden, values, seg_next, proj_bc, proj_dt, dt_bias, decay_rate, skip_gain,
          bc_prev, dt_prev, seg_prev, grad, gw):
    count = lax.axis_size("seq")
    tokens, heads = dt_prev.shape
    width = values.shape[1]
    dims = (tokens // SPAN, heads, gw // LANES, width // heads)
    npair = width // LANES
    half_pairs = npair // 2
    n = count // 2
    f32, bf16 = jnp.float32, jnp.bfloat16
    dma = pltpu.SemaphoreType.DMA
    wrows = proj_bc.shape[0]
    packed = wrows + LANES * LANES // gw
    nblocks = dims[0]
    work = [pltpu.VMEM((tokens, heads), f32), pltpu.VMEM((nblocks, heads, SPAN), f32),
            pltpu.VMEM((nblocks, heads, SPAN), f32), pltpu.VMEM((tokens, heads), f32)]
    kept = [pltpu.VMEM(s, f32) for s in ((npair, tokens, LANES), (npair, tokens, LANES),
                                         (nblocks + 1, npair, LANES, LANES), (nblocks + 1, npair, 1, LANES))]
    box = [pltpu.VMEM((half_pairs, LANES, LANES), bf16)] * 2
    gain = [pltpu.VMEM((npair, LANES), f32)] * 2
    half_gain = [pltpu.VMEM((half_pairs, LANES), f32)] * 2
    hbm = pl.BlockSpec(memory_space=pl.ANY)
    steps = n // 2
    staged = pl.pallas_call(
        functools.partial(fused_kernel, count, dims),
        out_shape=[jax.ShapeDtypeStruct(values.shape, bf16)] * 2,
        in_specs=[SM] * 2 + [VM] * 5 + [hbm] * 5,
        out_specs=[hbm] * 2,
        scratch_shapes=[
            pltpu.VMEM((tokens, hidden.shape[1]), bf16),
            pltpu.VMEM((n, 4, packed, gw), bf16), pltpu.VMEM((n, 4, wrows, gw), bf16),
            pltpu.VMEM((packed, gw), bf16), pltpu.VMEM((wrows, gw), bf16),
            pltpu.VMEM((tokens, width), bf16), pltpu.VMEM((tokens, width), bf16),
            *[pltpu.VMEM((tokens, gw), bf16)] * 4,
            pltpu.VMEM((tokens, 2 * gw + 2 * LANES), f32),
            pltpu.VMEM((tokens, heads), f32), pltpu.VMEM((tokens, heads), f32),
            pltpu.VMEM((1, heads), f32), pltpu.VMEM((1, heads), f32),
            *work, *work, *kept, *kept, *box * 9, *gain * 2, *half_gain * 2,
            dma((9,)), dma((2, steps, 2)), dma((2, steps, 4)), dma((n, 2)), dma((n, 2)),
            dma((2,)), dma((2,)), dma((2,)), dma((2,)), dma((4,)), dma((4,)),
            dma((2,)), dma((2, half_pairs)), dma((2,)), dma((2, half_pairs)),
            dma((2,)), dma((2, half_pairs // BATCH)), dma((2,)),
        ],
        compiler_params=pltpu.CompilerParams(
            collective_id=2, has_side_effects=True, vmem_limit_bytes=67_043_328),
        name="fused",
    )(seg_next, seg_prev, dt_bias[None], decay_rate[None], skip_gain[None], proj_dt, dt_prev.T,
      hidden, values, proj_bc, bc_prev, grad)
    chunk = pltpu.VMEM((tokens, width), bf16)
    return pl.pallas_call(
        hand_over,
        out_shape=[jax.ShapeDtypeStruct(values.shape, bf16)] * 2,
        in_specs=[hbm] * 2,
        out_specs=[hbm] * 2,
        scratch_shapes=[chunk, chunk, dma((2, HAND_PARTS)), dma((2,))],
        name="hand_over",
    )(*staged)


HAND_PARTS = 4


def hand_over(a_in, b_in, a_out, b_out, a_buf, b_buf, in_sem, out_sem):
    part = a_in.shape[0] // HAND_PARTS
    reads, writes = [], []
    for p in range(HAND_PARTS):
        rows = pl.ds(p * part, part)
        for k, (src, buf, dst) in enumerate(((a_in, a_buf, a_out), (b_in, b_buf, b_out))):
            reads.append(pltpu.make_async_copy(src.at[rows, :], buf.at[rows, :], in_sem.at[k, p]))
            writes.append(pltpu.make_async_copy(buf.at[rows, :], dst.at[rows, :], out_sem.at[k]))
    for copy in reads:
        copy.start()
    for read, write in zip(reads, writes):
        read.wait()
        write.start()
    for k, (buf, dst) in enumerate(((a_buf, a_out), (b_buf, b_out))):
        pltpu.make_async_copy(buf, dst, out_sem.at[k]).wait()


def body(
    hidden_next, values_next, seg_next, proj_bc, proj_dt, dt_bias, decay_rate, skip_gain,
    bc_prev, dt_prev, seg_prev, grad_prev,
):
    tokens_dev = hidden_next.shape[0]
    bc_width = proj_bc.shape[1]
    heads_all = proj_dt.shape[1]
    fsdp_count = lax.axis_size("fsdp")
    fsdp_place = lax.axis_index("fsdp")
    seq_count = lax.axis_size("seq")
    heads_dev = heads_all // fsdp_count
    state_dim = bc_width // (2 * GW)
    per_group = heads_all // GW
    groups_dev = max(1, heads_dev // per_group)
    first_head = fsdp_place * heads_dev
    first_group = first_head // per_group
    rows_dev = proj_bc.shape[0]
    half = bc_width // 2
    gw = groups_dev * state_dim

    if fsdp_count == 2 and seq_count % 4 == 0 and seq_count >= 8 and heads_all == LANES \
            and rows_dev == 2 * LANES and groups_dev * per_group == heads_dev:
        return fused(hidden_next, values_next, seg_next, proj_bc, proj_dt, dt_bias, decay_rate,
                     skip_gain, bc_prev, dt_prev, seg_prev, grad_prev, gw)

    blocks = []
    for f in range(fsdp_count):
        g0 = (f * heads_dev // per_group) * state_dim
        blocks.append([proj_bc[:, g0:g0 + gw], proj_bc[:, half + g0:half + g0 + gw]])
    ring = fsdp_count == 2 and seq_count % 4 == 0 and rows_dev % (2 * LANES) == 0 and heads_all == LANES
    if ring:
        shard = jnp.concatenate([*blocks[0], *blocks[1], proj_dt], axis=1)
        bc_next, dt_sum = gathered_sums(hidden_next, shard, 2 * gw)
        dt_sum = lax.dynamic_slice_in_dim(dt_sum, first_head, heads_dev, 1)
    else:
        pieces = []
        for f in range(fsdp_count):
            pieces += [*blocks[f], proj_dt[:, f * heads_dev:(f + 1) * heads_dev]]
        weights = lax.all_gather(jnp.concatenate(pieces, axis=1), "seq", axis=0, tiled=True)
        owned = lax.dynamic_slice_in_dim(
            hidden_next.reshape(tokens_dev, seq_count, fsdp_count, rows_dev), fsdp_place, 1, 2
        ).reshape(tokens_dev, seq_count * rows_dev)
        sums = lax.psum_scatter(jnp.dot(owned, weights, preferred_element_type=jnp.float32),
                                "fsdp", scatter_dimension=1, tiled=True)
        bc_next, dt_sum = sums[:, :2 * gw].astype(jnp.bfloat16), sums[:, 2 * gw:]

    decay = lax.dynamic_slice_in_dim(decay_rate, first_head, heads_dev, 0)[None]
    skip = lax.dynamic_slice_in_dim(skip_gain, first_head, heads_dev, 0)[None]
    bias = lax.dynamic_slice_in_dim(dt_bias, first_head, heads_dev, 0)[None]

    b_prev = lax.dynamic_slice_in_dim(bc_prev, first_group * state_dim, gw, 1)
    c_prev = lax.dynamic_slice_in_dim(bc_prev, half + first_group * state_dim, gw, 1)
    b_next, c_next = bc_next[:, :gw], bc_next[:, gw:]
    dt_next = jax.nn.softplus(dt_sum + bias)
    out_next, grad_values = chains(
        seg_next, values_next, c_next, b_next, dt_next, decay, skip,
        seg_prev, grad_prev, b_prev, c_prev, dt_prev)
    return (out_next, grad_values)


def solution(mesh):
    in_specs = (
        P("seq", None), P("seq", "fsdp"), P(), P(("seq", "fsdp"), None), P(("seq", "fsdp"), None),
        P(), P(), P(), P("seq", None), P("seq", "fsdp"), P(), P("seq", "fsdp"),
    )
    out_specs = (P("seq", "fsdp"), P("seq", "fsdp"))
    return jax.shard_map(body, mesh=mesh, in_specs=in_specs, out_specs=out_specs, check_vma=False)
```

```python
import functools

import jax
import jax.numpy as jnp
from jax import lax
from jax.experimental import pallas as pl
from jax.experimental.pallas import tpu as pltpu
from jax.sharding import PartitionSpec as P

GW = 4
SPAN = 128
LANES = 128
MESH = pl.DeviceIdType.MESH


def widen(a, c, head_dim):
    per = LANES // head_dim
    lane = lax.broadcasted_iota(jnp.int32, (1, LANES), 1)
    res = a[:, c * per:c * per + 1]
    for k in range(1, per):
        res = jnp.where(lane >= k * head_dim, a[:, c * per + k:c * per + k + 1], res)
    return jnp.broadcast_to(res, (a.shape[0], LANES))


def seg_maker(len_ref):
    bound = []
    total = jnp.int32(0)
    for k in range(len_ref.shape[0] - 1):
        total = total + len_ref[k]
        bound.append(total)

    def seg_of(pos):
        s = jnp.zeros_like(pos)
        for b in bound:
            s = s + (b <= pos).astype(jnp.int32)
        return s

    return seg_of


def local_states(back, dims, len_ref, x_ref, q_ref, dt_ref, decay_ref, work, pre, keep, part=None):
    nblocks, heads, groups, head_dim = dims
    cum_s, cum_t, dt_t, fout_s = work
    npair = heads * head_dim // LANES
    pair_group = npair // groups
    seg_of = seg_maker(len_ref)
    slab = lax.axis_index("seq") * (nblocks * SPAN)
    dim0 = lax.broadcasted_iota(jnp.int32, (SPAN, SPAN), 0)
    dim1 = lax.broadcasted_iota(jnp.int32, (SPAN, SPAN), 1)
    tril = (dim0 >= dim1).astype(jnp.float32)
    steps = range(nblocks) if part is None else part
    for c in range(npair if 0 in steps else 0):
        pre[0, c] = jnp.zeros((LANES, LANES), jnp.float32)
        keep[0, c] = jnp.ones((1, LANES), jnp.float32)
    for step in steps:
        b = nblocks - 1 - step if back else step
        rows = slice(b * SPAN, (b + 1) * SPAN)
        dt = dt_ref[rows, :]
        cum = jnp.dot(tril, -(dt * decay_ref[...]), precision=lax.Precision.HIGHEST,
                      preferred_element_type=jnp.float32)
        end = cum[SPAN - 1:SPAN, :]
        cum_s[rows, :] = cum
        cum_t[b] = cum.T
        dt_t[b] = dt.T
        seg = seg_of(slab + b * SPAN + lax.broadcasted_iota(jnp.int32, (SPAN, heads), 0))
        edge = slab + b * SPAN + lax.broadcasted_iota(jnp.int32, (1, heads), 0) * 0
        seg_e = seg_of(edge + (SPAN - 1))
        seg_b = jnp.where(edge == 0, 0, seg_of(edge - 1))
        send = jnp.where(seg == seg_e, jnp.exp(end - cum), 0.0) * dt
        read = jnp.where(seg == seg_b, jnp.exp(cum), 0.0)
        carry = jnp.where(seg_e == seg_b, jnp.exp(end), 0.0)
        f_in = read if back else send
        fout_s[rows, :] = send if back else read
        qt = [q_ref[rows, g * LANES:(g + 1) * LANES].T for g in range(groups)]
        for c in range(npair):
            cols = slice(c * LANES, (c + 1) * LANES)
            sent = (x_ref[rows, cols].astype(jnp.float32) * widen(f_in, c, head_dim)).astype(jnp.bfloat16)
            loc = jnp.dot(qt[c // pair_group], sent, preferred_element_type=jnp.float32)
            wide = widen(carry, c, head_dim)
            pre[step + 1, c] = wide * pre[step, c] + loc
            keep[step + 1, c] = wide * keep[step, c]


def in_block(back, dims, len_ref, x_ref, p_ref, q_ref, dt_ref, skip_ref, work, inside, fexp, span=None,
             only=None):
    nblocks, heads, groups, head_dim = dims
    cum_s, cum_t, dt_t, fout_s = work
    npair = heads * head_dim // LANES
    per = LANES // head_dim
    pair_group = npair // groups
    seg_of = seg_maker(len_ref)
    slab = lax.axis_index("seq") * (nblocks * SPAN)
    dim0 = lax.broadcasted_iota(jnp.int32, (SPAN, SPAN), 0)
    dim1 = lax.broadcasted_iota(jnp.int32, (SPAN, SPAN), 1)
    lane = lax.broadcasted_iota(jnp.int32, (1, LANES), 1)

    def one(b, _):
        start = pl.multiple_of(b * SPAN, SPAN)
        rows = pl.ds(start, SPAN)
        seg_i = seg_of(slab + start + dim0)
        seg_j = seg_of(slab + start + dim1)
        order = (dim1 >= dim0) if back else (dim1 <= dim0)
        bias = jnp.where((seg_i == seg_j) & order, 0.0, -jnp.inf)
        cum = cum_s[rows, :]
        dt = dt_ref[rows, :]
        f_out = fout_s[rows, :]
        for g in range(groups) if only is None else (only,):
            gl = slice(g * LANES, (g + 1) * LANES)
            score = lax.dot_general(p_ref[rows, gl], q_ref[rows, gl], (((1,), (1,)), ((), ())),
                                    preferred_element_type=jnp.float32)
            for c in range(g * pair_group, (g + 1) * pair_group):
                cols = slice(c * LANES, (c + 1) * LANES)
                x = x_ref[rows, cols]
                mixes, parts = [], []
                for k in range(per):
                    h = c * per + k
                    col = cum[:, h:h + 1]
                    row = cum_t[b, h:h + 1, :]
                    spread = (row - col) if back else (col - row)
                    w = jnp.exp(spread + bias) * score
                    if not back:
                        w = w * dt_t[b, h:h + 1, :]
                    mixes.append(w.astype(jnp.bfloat16))
                    mine = (lane >= k * head_dim) & (lane < (k + 1) * head_dim)
                    parts.append(jnp.where(mine, x, jnp.zeros_like(x)))
                acc = jnp.dot(jnp.concatenate(mixes, 1), jnp.concatenate(parts, 0),
                              preferred_element_type=jnp.float32)
                if back:
                    acc = acc * widen(dt, c, head_dim)
                inside[c, rows, :] = acc + widen(skip_ref[...], c, head_dim) * x.astype(jnp.float32)
                fexp[c, rows, :] = widen(f_out, c, head_dim)
        return 0

    first, last = (0, nblocks) if span is None else span
    lax.fori_loop(first, last, one, 0)


HOP_CHUNKS = 5


def chain_kernel(count, dims, len_ref, x_ref, p_ref, q_ref, dt_ref, decay_ref, skip_ref,
                 lenb_ref, xb_ref, pb_ref, qb_ref, dtb_ref,
                 out_ref, grad_ref, *scratch):
    work, work_b, rest = scratch[:4], scratch[4:8], scratch[12:]
    inside_b, fexp_b, pre_b, keep_b = scratch[8:12]
    inside, fexp, pre, keep, inbox, outbox, in_b, out_b, s_sem, r_sem, sb_sem, rb_sem = rest
    nblocks, heads, groups, head_dim = dims
    npair = heads * head_dim // LANES
    pair_group = npair // groups
    me = lax.axis_index("seq")
    low, high = me == 0, me == count - 1

    barrier = pltpu.get_barrier_semaphore()

    @pl.when(jnp.logical_not(low))
    def _():
        pl.semaphore_signal(barrier, inc=1, device_id={"seq": me - 1}, device_id_type=MESH)

    @pl.when(jnp.logical_not(high))
    def _():
        pl.semaphore_signal(barrier, inc=1, device_id={"seq": me + 1}, device_id_type=MESH)

    local_states(False, dims, len_ref, x_ref, q_ref, dt_ref, decay_ref, work, pre, keep)
    local_states(True, dims, lenb_ref, xb_ref, qb_ref, dtb_ref, decay_ref, work_b, pre_b, keep_b)

    @pl.when(low)
    def _():
        inbox[...] = jnp.zeros_like(inbox)

    @pl.when(high)
    def _():
        in_b[...] = jnp.zeros_like(in_b)

    pl.semaphore_wait(barrier, jnp.where(low, 0, 1) + jnp.where(high, 0, 1))

    def hop(back, c):
        return pltpu.make_async_remote_copy(
            src_ref=(out_b if back else outbox).at[c], dst_ref=(in_b if back else inbox).at[c],
            send_sem=(sb_sem if back else s_sem).at[c], recv_sem=(rb_sem if back else r_sem).at[c],
            device_id={"seq": me - 1 if back else me + 1}, device_id_type=MESH)

    def relay(back, c):
        first, last = (high, low) if back else (low, high)
        kp, pr = (keep_b, pre_b) if back else (keep, pre)

        @pl.when(jnp.logical_not(first))
        def _():
            hop(back, c).wait_recv()

        @pl.when(jnp.logical_not(last))
        def _():
            state = (in_b if back else inbox)[c].astype(jnp.float32)
            (out_b if back else outbox)[c] = (kp[nblocks, c] * state + pr[nblocks, c]).astype(jnp.bfloat16)
            hop(back, c).start()

    def finish(back, c):
        kp, pr, ins, fx, vec, out = (
            (keep_b, pre_b, inside_b, fexp_b, pb_ref, grad_ref) if back
            else (keep, pre, inside, fexp, p_ref, out_ref))
        g = c // pair_group
        cols = pl.ds(pl.multiple_of(c * LANES, LANES), LANES)
        gl = pl.ds(pl.multiple_of(g * LANES, LANES), LANES)
        state = (in_b if back else inbox)[c].astype(jnp.float32)
        for step in range(nblocks):
            b = nblocks - 1 - step if back else step
            rows = slice(b * SPAN, (b + 1) * SPAN)
            entering = (kp[step, c] * state + pr[step, c]).astype(jnp.bfloat16)
            y = jnp.dot(vec[rows, gl], entering, preferred_element_type=jnp.float32)
            out[rows, cols] = (ins[c, rows, :] + fx[c, rows, :] * y).astype(jnp.bfloat16)

    lag = (2 * me - (count - 1)) * HOP_CHUNKS
    up_first = lag < 0
    gap = jnp.where(up_first, -lag, lag)
    block_at = jnp.where(gap >= npair, npair, 0)

    def step_of(i, _):
        @pl.when(i == block_at)
        def _():
            in_block(False, dims, len_ref, x_ref, p_ref, q_ref, dt_ref, skip_ref, work, inside, fexp)
            in_block(True, dims, lenb_ref, xb_ref, pb_ref, qb_ref, dtb_ref, skip_ref, work_b, inside_b, fexp_b)

        for back in (False, True):
            leads = jnp.logical_not(up_first) if back else up_first
            c = i - jnp.where(leads, 0, gap)

            @pl.when((c >= 0) & (c < npair))
            def _(back=back, c=c):
                relay(back, c)

            done = jnp.where(leads, i - npair, c)

            @pl.when((done >= 0) & (done < npair))
            def _(back=back, done=done):
                finish(back, done)

        return 0

    lax.fori_loop(0, npair + jnp.maximum(gap, npair), step_of, 0)

    def drain(c, _):
        @pl.when(jnp.logical_not(high))
        def _():
            hop(False, c).wait_send()

        @pl.when(jnp.logical_not(low))
        def _():
            hop(True, c).wait_send()

        return 0

    lax.fori_loop(0, npair, drain, 0)


def sizes_of(x, p_vec, dt):
    tokens, width = x.shape
    heads = dt.shape[1]
    dims = (tokens // SPAN, heads, p_vec.shape[1] // LANES, width // heads)
    nblocks, npair = dims[0], width // LANES
    f32 = jnp.float32
    work = [pltpu.VMEM((tokens, heads), f32), pltpu.VMEM((nblocks, heads, SPAN), f32),
            pltpu.VMEM((nblocks, heads, SPAN), f32), pltpu.VMEM((tokens, heads), f32)]
    kept = [(npair, tokens, LANES), (npair, tokens, LANES),
            (nblocks + 1, npair, LANES, LANES), (nblocks + 1, npair, 1, LANES)]
    return dims, npair, work, kept


VM = pl.BlockSpec(memory_space=pltpu.VMEM)
SM = pl.BlockSpec(memory_space=pltpu.SMEM)


def chains(lengths, x, p_vec, q_vec, dt, decay, skip, *back):
    dims, npair, work, kept = sizes_of(x, p_vec, dt)
    box = pltpu.VMEM((npair, LANES, LANES), jnp.bfloat16)
    sem = pltpu.SemaphoreType.DMA((npair,))
    return pl.pallas_call(
        functools.partial(chain_kernel, lax.axis_size("seq"), dims),
        out_shape=[jax.ShapeDtypeStruct(x.shape, jnp.bfloat16)] * 2,
        in_specs=[SM] + [VM] * 6 + [SM] + [VM] * 4,
        out_specs=[VM] * 2,
        scratch_shapes=(work * 2 + [pltpu.VMEM(k, jnp.float32) for k in kept] * 2
                        + [box] * 4 + [sem] * 4),
        compiler_params=pltpu.CompilerParams(
            collective_id=0, has_side_effects=True, vmem_limit_bytes=56 * 1024 * 1024),
        cost_estimate=pl.CostEstimate(flops=40_000_000_000, bytes_accessed=40_000_000, transcendentals=0),
        name="chains",
    )(lengths, x, p_vec, q_vec, dt, decay, skip, *back)


PIECES = 4


def gather_kernel(count, h_ref, w_ref, bc_ref, dt_ref,
                  held, acc, bc_out, bc_in, dt_out, dt_in,
                  ring_s, ring_r, side_s, side_r, x_s, x_r):
    me, f = lax.axis_index("seq"), lax.axis_index("fsdp")
    n = count // 2
    half_ring = n // 2
    core, chip = me % 2, me // 2
    r = jnp.where(chip % 2 == 0, chip // 2, n - 1 - chip // 2)
    rows = w_ref.shape[0]
    piece = rows // PIECES
    wide = bc_ref.shape[1]

    def id_of(pos, which):
        p = (pos + 2 * n) % n
        up = p < half_ring
        return jnp.where(up, p * 2, (n - 1 - p) * 2 + 1) * 2 + which

    nxt, prv, partner = id_of(r + 1, core), id_of(r - 1, core), chip * 2 + 1 - core

    barrier = pltpu.get_barrier_semaphore()
    for peer in (nxt, prv, partner):
        pl.semaphore_signal(barrier, inc=1, device_id={"seq": peer}, device_id_type=MESH)
    pl.semaphore_signal(barrier, inc=1, device_id={"fsdp": 1 - f}, device_id_type=MESH)
    pl.semaphore_wait(barrier, 4)

    def part(p):
        return pl.ds(p * piece, piece)

    def origin(step, p, which):
        return id_of(r - step if p < PIECES // 2 else r + step, which)

    def ring_copy(step, p, src):
        return pltpu.make_async_remote_copy(
            src_ref=src, dst_ref=held.at[origin(step, p, core), part(p), :],
            send_sem=ring_s.at[step, p], recv_sem=ring_r.at[step, p],
            device_id={"seq": nxt if p < PIECES // 2 else prv}, device_id_type=MESH)

    def side_copy(step, p, src):
        return pltpu.make_async_remote_copy(
            src_ref=src, dst_ref=held.at[origin(step, p, core), part(p), :],
            send_sem=side_s.at[step, p], recv_sem=side_r.at[step, p],
            device_id={"seq": partner}, device_id_type=MESH)

    def landed(step, p):
        return held.at[origin(step, p, core), part(p), :]

    for p in range(PIECES):
        ring_copy(0, p, w_ref.at[part(p), :]).start()
    for p in range(PIECES):
        side_copy(0, p, w_ref.at[part(p), :]).start()

    def columns(seq_index, first):
        start = (seq_index * 2 + f) * rows + first
        return h_ref[:, pl.ds(pl.multiple_of(start, rows // 2), rows // 2)]

    def mac(step, which):
        half = rows // 2
        lo, hi = origin(step, 0, which), origin(step, PIECES - 1, which)
        left = jnp.concatenate([columns(lo, 0), columns(hi, half)], axis=1)
        right = jnp.concatenate([held[lo, 0:half, :], held[hi, half:, :]], axis=0)
        acc[...] += jnp.dot(left, right, preferred_element_type=jnp.float32)

    acc[...] = jnp.dot(jnp.concatenate([columns(me, 0), columns(me, rows // 2)], axis=1), w_ref[...],
                       preferred_element_type=jnp.float32)

    def one(step, _):
        for p in (0, PIECES // 2, 1, PIECES // 2 + 1):
            ring_copy(step, p, landed(step, p)).wait_recv()

            @pl.when(step < n - 2)
            def _(p=p):
                ring_copy(step + 1, p, landed(step + 1, p)).start()

            side_copy(step + 1, p, landed(step + 1, p)).start()
        mac(step + 1, core)
        for p in range(PIECES):
            side_copy(step, p, landed(step, p)).wait_recv()
        mac(step, 1 - core)
        return 0

    lax.fori_loop(0, n - 1, one, 0)
    for p in range(PIECES):
        side_copy(n - 1, p, landed(n - 1, p)).wait_recv()
    mac(n - 1, 1 - core)

    def cross(src, dst, k):
        return pltpu.make_async_remote_copy(
            src_ref=src, dst_ref=dst, send_sem=x_s.at[k], recv_sem=x_r.at[k],
            device_id={"fsdp": 1 - f}, device_id_type=MESH)

    def side_of(which):
        return pl.ds(pl.multiple_of(which * wide, wide), wide)

    bc_out[...] = acc[:, side_of(1 - f)]
    dt_out[...] = acc[:, 2 * wide:]
    cross(bc_out, bc_in, 0).start()
    cross(dt_out, dt_in, 1).start()

    def drain(step, _):
        for p in range(PIECES):
            @pl.when(step < n - 1)
            def _(p=p):
                ring_copy(step, p, landed(step, p)).wait_send()

            side_copy(step, p, landed(step, p)).wait_send()
        return 0

    lax.fori_loop(0, n, drain, 0)
    cross(bc_out, bc_in, 0).wait()
    bc_ref[...] = (acc[:, side_of(f)] + bc_in[...]).astype(jnp.bfloat16)
    cross(dt_out, dt_in, 1).wait()
    dt_ref[...] = acc[:, 2 * wide:] + dt_in[...]


def gathered_sums(hidden, shard, wide):
    count = lax.axis_size("seq")
    tokens, total = hidden.shape[0], shard.shape[1]
    f32, bf16 = jnp.float32, jnp.bfloat16
    n = count // 2
    dma = pltpu.SemaphoreType.DMA
    return pl.pallas_call(
        functools.partial(gather_kernel, count),
        out_shape=[jax.ShapeDtypeStruct((tokens, wide), bf16),
                   jax.ShapeDtypeStruct((tokens, total - 2 * wide), f32)],
        in_specs=[VM] * 2,
        out_specs=[VM] * 2,
        scratch_shapes=[
            pltpu.VMEM((count,) + shard.shape, bf16),
            pltpu.VMEM((tokens, total), f32),
            pltpu.VMEM((tokens, wide), f32), pltpu.VMEM((tokens, wide), f32),
            pltpu.VMEM((tokens, total - 2 * wide), f32), pltpu.VMEM((tokens, total - 2 * wide), f32),
            dma((n, PIECES)), dma((n, PIECES)), dma((n, PIECES)), dma((n, PIECES)), dma((2,)), dma((2,)),
        ],
        compiler_params=pltpu.CompilerParams(
            collective_id=1, has_side_effects=True, vmem_limit_bytes=32 * 1024 * 1024),
        cost_estimate=pl.CostEstimate(flops=40_000_000_000, bytes_accessed=40_000_000, transcendentals=0),
        name="gather_project",
    )(hidden, shard)


Z_LAG = 6
BLOCK_GAP = 3
CORE_LAG = 3
BATCH = 4
EARLY = 0


def fused_kernel(count, dims, len_ref, lenb_ref, bias_in, decay_in, skip_in, pdt_ref, dtt_ref,
                 h_hbm, x_hbm, w_hbm, bcp_hbm, g_hbm, out_hbm, grad_hbm,
                 hid, held_b, held_c, yout_b, yout_c, xv, gv, bp, cp, bn, cn, acc, dtn, dtp, decay_ref, skip_ref,
                 *scratch):
    work, work_b = scratch[:4], scratch[4:8]
    kept = (scratch[8:12], scratch[12:16])
    lout, lin, xout, xin, zout, zin, eout, ein, eown, kv, ksib, kxo, kxi = (
        (scratch[16 + 2 * i], scratch[17 + 2 * i]) for i in range(13))
    (ld, ring_s, ring_r, side_s, side_r, y_s, y_r, l_s, l_r, k_s, k_r, c_s, c_r, z_s, z_r,
     e_s, e_r, o_sem) = scratch[42:]
    nblocks, heads, groups, head_dim = dims
    npair = heads * head_dim // LANES
    pair_group = npair // groups
    half_pairs = npair // 2
    me, f = lax.axis_index("seq"), lax.axis_index("fsdp")
    core, chip = me % 2, me // 2
    xpos, zpos, nz = chip % 2, chip // 2, count // 4
    n = count // 2
    half_ring = n // 2
    full = half_ring - 1
    far = 2 * full + 1
    gw = groups * LANES
    wrows = w_hbm.shape[0]
    r = jnp.where(xpos == 0, zpos, n - 1 - zpos)

    def chip_at(pos):
        p = (pos + 2 * n) % n
        return jnp.where(p < half_ring, p * 2, (n - 1 - p) * 2 + 1)

    nxt, prv = chip_at(r + 1) * 2 + core, chip_at(r - 1) * 2 + core
    partner = chip * 2 + 1 - core
    xpeer = (zpos * 2 + 1 - xpos) * 2 + core
    own, other = core * 2 + f, core * 2 + 1 - f

    def at_cols(start):
        return pl.ds(pl.multiple_of(start, LANES), gw)

    def load(src, dst, k):
        return pltpu.make_async_copy(src, dst, ld.at[k])

    w_half = w_hbm.shape[1] // 2
    w_loads = [
        load(w_hbm.at[:, at_cols(f * gw)], held_b.at[chip, own, 0:wrows, :], 0),
        load(w_hbm.at[:, at_cols((1 - f) * gw)], yout_b.at[0:wrows, :], 1),
        load(w_hbm.at[:, at_cols(w_half + f * gw)], held_c.at[chip, own, :, :], 2),
        load(w_hbm.at[:, at_cols(w_half + (1 - f) * gw)], yout_c, 3),
    ]
    b_loads = [
        load(g_hbm, gv, 4),
        load(bcp_hbm.at[:, at_cols(f * gw)], bp, 5),
        load(bcp_hbm.at[:, at_cols(w_half + f * gw)], cp, 6),
    ]
    h_load, x_load = load(h_hbm, hid, 7), load(x_hbm, xv, 8)
    for copy in (*w_loads, *b_loads, h_load, x_load):
        copy.start()

    barrier = pltpu.get_barrier_semaphore()
    for peer in (partner, xpeer):
        pl.semaphore_signal(barrier, inc=1, device_id={"seq": peer}, device_id_type=MESH)
    pl.semaphore_signal(barrier, inc=1, device_id={"fsdp": 1 - f}, device_id_type=MESH)

    @pl.when(zpos > 0)
    def _():
        pl.semaphore_signal(barrier, inc=1, device_id={"seq": me - 4}, device_id_type=MESH)

    @pl.when(zpos < nz - 1)
    def _():
        pl.semaphore_signal(barrier, inc=1, device_id={"seq": me + 4}, device_id_type=MESH)

    lane = lax.broadcasted_iota(jnp.int32, (LANES, LANES), 1)
    top = pdt_ref[0:LANES, :].astype(jnp.float32)
    low = pdt_ref[LANES:2 * LANES, :].astype(jnp.float32)
    pack0 = jnp.where(lane < heads, top, pltpu.roll(low, heads, 1))
    pack1 = jnp.where(lane < heads, pltpu.roll(top, heads, 1), low)
    mine = jnp.where(f == 0, pack0, pack1).astype(jnp.bfloat16)
    theirs = jnp.where(f == 0, pack1, pack0).astype(jnp.bfloat16)
    strips = gw // LANES
    strip = LANES // strips
    for k in range(strips):
        lanes = slice(k * LANES, (k + 1) * LANES)
        held_b[chip, own, wrows:wrows + strip, lanes] = mine[k * strip:(k + 1) * strip, :]
        yout_b[wrows:wrows + strip, lanes] = theirs[k * strip:(k + 1) * strip, :]
    decay_ref[...] = jnp.where(f == 0, decay_in[:, 0:heads], decay_in[:, heads:2 * heads])
    skip_ref[...] = jnp.where(f == 0, skip_in[:, 0:heads], skip_in[:, heads:2 * heads])
    bias = jnp.where(f == 0, bias_in[:, 0:heads], bias_in[:, heads:2 * heads])
    for b in range(nblocks):
        dtp[b * SPAN:(b + 1) * SPAN, :] = dtt_ref[:, b * SPAN:(b + 1) * SPAN].T

    pl.semaphore_wait(barrier, 3 + jnp.where(zpos > 0, 1, 0) + jnp.where(zpos < nz - 1, 1, 0))
    for copy in w_loads:
        copy.wait()

    def piece(where, j, mine=True):
        base = (core if mine else 1 - core) * 2
        return (held_b if j < 2 else held_c).at[where, base + (f if j % 2 == 0 else 1 - f)]

    def remote(src, dst, s, rv, **peer):
        return pltpu.make_async_remote_copy(src_ref=src, dst_ref=dst, send_sem=s, recv_sem=rv,
                                            device_id=peer, device_id_type=MESH)

    def ring(d, k, j, arrived=False):
        away = k if arrived else k - 1
        ref = piece(chip_at(r - away if d == 0 else r + away), j)
        return remote(ref, ref, ring_s.at[d, k - 1, j // 2], ring_r.at[d, k - 1, j],
                      seq=nxt if d == 0 else prv)

    def chip_of(u):
        return chip_at(r - u if u <= full else (r + (u - full) if u < far else r + half_ring))

    def side(u, j):
        ref = piece(chip_of(u), j)
        return remote(ref, ref, side_s.at[u, j // 2], side_r.at[u, j // 2], seq=partner)

    def both(where, kind, mine=True):
        return (held_c if kind else held_b).at[where, pl.ds((core if mine else 1 - core) * 2, 2)]

    def side_both(u, kind, arrived=False):
        ref = both(chip_of(u), kind, not arrived)
        return remote(ref, ref, side_s.at[u, kind], side_r.at[u, kind], seq=partner)

    def cross(kind, arrived=False):
        ref = held_c if kind else held_b
        return remote(yout_c if kind else yout_b, ref.at[chip, other if arrived else own],
                      y_s.at[kind], y_r.at[kind], fsdp=1 - f)

    def begin(j):
        ring(0, 1, j).start()
        ring(1, 1, j).start()
        side(0, j).start()

    for kind in range(2):
        cross(kind).start()
        begin(2 * kind)

    def receive(k, kind, second=False):
        for d in range(2):
            if k > full and second:
                continue
            j = 2 * kind + ((1 - d if second else d) if k > 1 or kind else int(second))
            ring(d, k, j, True).wait_recv()
            if k < full or (k == full and j % 2 == d):
                ring(d, k + 1, j).start()
            side(far if k > full else (k if d == 0 else full + k), j).start()

    wide = 4 * wrows

    def add(at, value, first):
        cols = slice(at, at + value.shape[1])
        acc[:, cols] = value if first else acc[:, cols] + value

    def mac(u, kind, first=False):
        side_both(u, kind, True).wait_recv()
        q = chip_of(u)
        left = hid[:, pl.ds(pl.multiple_of(q * wide, wide), wide)]
        ref = held_c if kind else held_b
        add(gw + 2 * LANES if kind else 0,
            jnp.dot(left, jnp.concatenate([ref[q, s, 0:wrows, :] for s in range(4)], axis=0),
                    preferred_element_type=jnp.float32), first)
        if kind == 0:
            packs = jnp.concatenate(
                [held_b[q, s, wrows:wrows + strip, k * LANES:(k + 1) * LANES]
                 for s in range(4) for k in range(strips)], axis=0)
            for o in range(2):
                part = jnp.concatenate(
                    [left[:, s * wrows + o * LANES:s * wrows + (o + 1) * LANES] for s in range(4)], axis=1)
                add(gw + o * LANES, jnp.dot(part, packs, preferred_element_type=jnp.float32), first)

    def l_copy(back):
        return remote(lout[back], lin[back], l_s.at[back], l_r.at[back], seq=partner)

    def exchange(back):
        pre, keep = kept[back][2:]
        for c in range(npair):
            kv[back][c:c + 1, :] = keep[nblocks, c]
        remote(kv[back], ksib[back], k_s.at[back], k_r.at[back], seq=partner).start()

        def put(i, _):
            lout[back][i] = pre[nblocks, (1 - core) * half_pairs + i].astype(jnp.bfloat16)
            return 0

        lax.fori_loop(0, half_pairs, put, 0)
        l_copy(back).start()

    def lead_core(back):
        return (core == 1) if back else (core == 0)

    def lead_x(back):
        return (xpos == 1) if back else (xpos == 0)

    def ends(back):
        return (zpos == 0) if back else (zpos == nz - 1)

    def gives(back):
        return jnp.logical_not(ends(back)) | lead_x(back)

    def takes(back):
        return jnp.logical_not(ends(back) & lead_x(back))

    def row(ref, i):
        return ref[pl.ds(i, 1), :]

    def x_copy(back, i):
        return remote(xout[back].at[i], xin[back].at[i], c_s.at[back], c_r.at[back, i], seq=xpeer)

    def kx_copy(back):
        return remote(kxo[back], kxi[back], k_s.at[2 + back], k_r.at[2 + back], seq=xpeer)

    def combine(back):
        rows = pl.ds(pl.multiple_of(core * half_pairs, half_pairs), half_pairs)
        remote(kv[back], ksib[back], k_s.at[back], k_r.at[back], seq=partner).wait_recv()
        kxo[back][...] = kv[back][rows, :] * ksib[back][rows, :]
        sends = gives(back)

        @pl.when(sends)
        def _():
            kx_copy(back).start()

    def combine_part(back, send):
        l_copy(back).wait_recv()
        pre = kept[back][2]
        sends = gives(back)

        def put(i, _):
            g = core * half_pairs + i
            lead = lead_core(back)
            total = (pre[nblocks, g] * jnp.where(lead, row(ksib[back], g), 1.0)
                     + lin[back][i].astype(jnp.float32) * jnp.where(lead, 1.0, row(kv[back], g)))
            xout[back][i] = total.astype(jnp.bfloat16)
            if send:
                @pl.when(sends)
                def _():
                    x_copy(back, i).start()

            return 0

        lax.fori_loop(0, half_pairs, put, 0)

    def x_sends(back, start, stop):
        def put(i, _):
            x_copy(back, i).start()
            return 0

        @pl.when(gives(back))
        def _():
            lax.fori_loop(start, stop, put, 0)

    def z_copy(back, i):
        return remote(zout[back].at[i], zin[back].at[i], z_s.at[back], z_r.at[back, i],
                      seq=me - 4 if back else me + 4)

    def e_copy(back, k):
        part = pl.ds(k * BATCH, BATCH)
        return remote(eout[back].at[part], ein[back].at[part], e_s.at[back], e_r.at[back, k], seq=partner)

    def out_copy(back, k):
        cols = pl.ds(pl.multiple_of(k * BATCH * LANES, LANES), BATCH * LANES)
        src, dst = (gv, grad_hbm) if back else (xv, out_hbm)
        return pltpu.make_async_copy(src.at[:, cols], dst.at[:, cols], o_sem.at[back])

    def finish(back, c0, states, i0):
        ins, fx, pre, keep = kept[back]
        vec, out = (bp, gv) if back else (cn, xv)
        gl = pl.ds(pl.multiple_of((c0 // pair_group) * LANES, LANES), LANES)
        for step in range(nblocks):
            b = nblocks - 1 - step if back else step
            rows = slice(b * SPAN, (b + 1) * SPAN)
            for k in range(0, BATCH, 2):
                entering = []
                for c, i in ((c0 + k, i0 + k), (c0 + k + 1, i0 + k + 1)):
                    state = states[i]
                    if step > 0:
                        state = (keep[step, c] * state.astype(jnp.float32) + pre[step, c]).astype(jnp.bfloat16)
                    entering.append(state)
                y = jnp.dot(vec[rows, gl], jnp.concatenate(entering, axis=1), preferred_element_type=jnp.float32)
                for m in range(2):
                    c = c0 + k + m
                    cols = pl.ds(pl.multiple_of(c * LANES, LANES), LANES)
                    part = y[:, m * LANES:(m + 1) * LANES]
                    out[rows, cols] = (ins[c, rows, :] + fx[c, rows, :] * part).astype(jnp.bfloat16)
        out_copy(back, c0 // BATCH).start()

    def relay(back, i):
        pre = kept[back][2]
        g = core * half_pairs + i
        z_first, z_last = (zpos == nz - 1, zpos == 0) if back else (zpos == 0, zpos == nz - 1)

        @pl.when((i == 0) & takes(back))
        def _():
            kx_copy(back).wait_recv()

        @pl.when((i == 0) & jnp.logical_not(takes(back)))
        def _():
            kxi[back][...] = jnp.zeros_like(kxi[back])

        @pl.when(takes(back))
        def _():
            x_copy(back, i).wait_recv()

        @pl.when(jnp.logical_not(z_first))
        def _():
            z_copy(back, i).wait_recv()

        k_own, k_peer = row(kxo[back], i), row(kxi[back], i)
        l_own = xout[back][i].astype(jnp.float32)
        l_peer = jnp.where(takes(back), xin[back][i].astype(jnp.float32), 0.0)
        state = jnp.where(z_first, 0.0, zin[back][i].astype(jnp.float32))
        lead = lead_x(back)
        zout[back][i] = (k_own * k_peer * state + l_own * jnp.where(lead, k_peer, 1.0)
                         + l_peer * jnp.where(lead, 1.0, k_own)).astype(jnp.bfloat16)

        @pl.when(jnp.logical_not(z_last))
        def _():
            z_copy(back, i).start()

        state = jnp.where(lead, state, k_peer * state + l_peer)
        head = lead_core(back)
        k_lead = jnp.where(head, row(kv[back], g), row(ksib[back], g))
        l_lead = jnp.where(head, pre[nblocks, g], lin[back][i].astype(jnp.float32))
        after = k_lead * state + l_lead
        eout[back][i] = jnp.where(head, after, state).astype(jnp.bfloat16)

        @pl.when(i % BATCH == BATCH - 1)
        def _():
            e_copy(back, i // BATCH).start()

        eown[back][i] = jnp.where(head, state, after).astype(jnp.bfloat16)

    def settle(back, i):
        e_copy(back, i // BATCH).wait_recv()
        finish(back, core * half_pairs + i, eown[back], i)
        finish(back, (1 - core) * half_pairs + i, ein[back], i)

    def block(back, b):
        if back:
            in_block(True, dims, lenb_ref, gv, bp, cp, dtp, skip_ref, work_b, *kept[1][:2], span=(b, b + 1))
        else:
            at, g = b
            in_block(False, dims, len_ref, xv, cn, bn, dtn, skip_ref, work, *kept[0][:2],
                     span=(at, at + 1), only=g)

    for copy in b_loads:
        copy.wait()
    local_states(True, dims, lenb_ref, gv, cp, dtp, decay_ref, work_b, *kept[1][2:])
    for kind in range(2):
        cross(kind, True).wait_recv()
        begin(2 * kind + 1)
    receive(1, 0)
    exchange(1)
    block(True, 0)
    receive(1, 0, True)
    receive(1, 1)
    block(True, 1)
    combine(1)
    combine_part(1, False)
    outer = (zpos == 0) | (zpos == nz - 1)
    x_sends(1, 0, jnp.where(outer, 0, half_pairs))
    h_load.wait()
    mac(0, 0, True)
    c_next = [(k, second) for k in range(1, full + 1) for second in (False, True)][1:]
    for k in range(2, full + 1):
        receive(k, 0)
        receive(k, 0, True)
        if k == 2:
            mac(0, 1, True)
        for u in (k - 1, full + k - 1):
            mac(u, 0)
        for _ in range(2 if k == full else 1):
            step, second = c_next.pop(0)
            receive(step, 1, second)
        if k == 2:
            for u in (1, full + 1):
                mac(u, 1)
    for u in (full, 2 * full):
        mac(u, 0)
    receive(full + 1, 0)
    x_load.wait()
    mac(far, 0)
    at = gw
    bn[...] = acc[:, 0:gw].astype(jnp.bfloat16)
    dt_sum = acc[:, at:at + heads] + acc[:, at + LANES + heads:at + LANES + 2 * heads] + bias
    dtn[...] = jnp.maximum(dt_sum, 0.0) + jnp.log1p(jnp.exp(-jnp.abs(dt_sum)))

    def forward_states(steps):
        local_states(False, dims, len_ref, xv, bn, dtn, decay_ref, work, *kept[0][2:], part=steps)

    forward_states((0,))
    while len(c_next) > 1:
        step, second = c_next.pop(0)
        receive(step, 1, second)
    early = jnp.where(zpos == 0, EARLY, half_pairs)
    x_sends(1, jnp.where(outer, 0, half_pairs), early)
    forward_states(range(1, nblocks))
    exchange(0)
    for step, second in c_next:
        receive(step, 1, second)
    for u in (2, full + 2):
        mac(u, 1)
    combine(0)
    combine_part(0, True)
    x_sends(1, early, half_pairs)
    for k in range(3, full + 1):
        for u in (k, full + k):
            mac(u, 1)
    receive(full + 1, 1)
    mac(far, 1)
    cn[...] = acc[:, gw + 2 * LANES:].astype(jnp.bfloat16)
    block_end = 1 + BLOCK_GAP * (groups * nblocks - 1)

    def tick(t, _):
        for back in range(2):
            i = t - ((nz - 1 - zpos) if back else zpos) * Z_LAG

            @pl.when((i >= 0) & (i < half_pairs))
            def _(back=back, i=i):
                relay(back, i)

        for g in range(groups):
            u = (t - 1) // BLOCK_GAP - g * nblocks

            @pl.when(((t - 1) % BLOCK_GAP == 0) & (u >= 0) & (u < nblocks))
            def _(u=u, g=g):
                block(False, (u, g))

        for back in range(2):
            lag = ((nz - 1 - zpos) if back else zpos) * Z_LAG + CORE_LAG
            late = t - (lag if back else jnp.maximum(lag, block_end + 2 - BATCH))

            @pl.when((late >= 0) & (late < half_pairs) & (late % BATCH == BATCH - 1))
            def _(back=back, late=late):
                settle(back, late - (BATCH - 1))

        return 0

    last = max(half_pairs + CORE_LAG + (nz - 1) * Z_LAG, half_pairs + block_end + 2 - BATCH)
    lax.fori_loop(0, last, tick, 0)

    for j in range(2):
        cross(j).wait_send()
    for k in range(1, half_ring + 1):
        for d in range(2):
            for kind in range(2):
                if k > full:
                    ring(d, k, 2 * kind + d).wait_send()
                else:
                    ref = both(chip, kind)
                    remote(ref, ref, ring_s.at[d, k - 1, kind], ring_r.at[d, k - 1, 2 * kind],
                           seq=partner).wait_send()
    for u in range(far + 1):
        for kind in range(2):
            side_both(u, kind).wait_send()
    for back in range(2):
        remote(kv[back], ksib[back], k_s.at[back], k_r.at[back], seq=partner).wait_send()
        given = gives(back)

        @pl.when(given)
        def _(back=back):
            kx_copy(back).wait_send()

        @pl.when(given)
        def _(back=back):
            remote(xout[back], xin[back], c_s.at[back], c_r.at[back, 0], seq=xpeer).wait_send()

        @pl.when(zpos != (0 if back else nz - 1))
        def _(back=back):
            remote(zout[back], zin[back], z_s.at[back], z_r.at[back, 0], seq=xpeer).wait_send()

        l_copy(back).wait_send()
        remote(eout[back], ein[back], e_s.at[back], e_r.at[back, 0], seq=partner).wait_send()
        pltpu.make_async_copy(*((gv, grad_hbm) if back else (xv, out_hbm)), o_sem.at[back]).wait()


def fused(hidden, values, seg_next, proj_bc, proj_dt, dt_bias, decay_rate, skip_gain,
          bc_prev, dt_prev, seg_prev, grad, gw):
    count = lax.axis_size("seq")
    tokens, heads = dt_prev.shape
    width = values.shape[1]
    dims = (tokens // SPAN, heads, gw // LANES, width // heads)
    npair = width // LANES
    half_pairs = npair // 2
    n = count // 2
    f32, bf16 = jnp.float32, jnp.bfloat16
    dma = pltpu.SemaphoreType.DMA
    wrows = proj_bc.shape[0]
    packed = wrows + LANES * LANES // gw
    nblocks = dims[0]
    work = [pltpu.VMEM((tokens, heads), f32), pltpu.VMEM((nblocks, heads, SPAN), f32),
            pltpu.VMEM((nblocks, heads, SPAN), f32), pltpu.VMEM((tokens, heads), f32)]
    kept = [pltpu.VMEM(s, f32) for s in ((npair, tokens, LANES), (npair, tokens, LANES),
                                         (nblocks + 1, npair, LANES, LANES), (nblocks + 1, npair, 1, LANES))]
    box = [pltpu.VMEM((half_pairs, LANES, LANES), bf16)] * 2
    gain = [pltpu.VMEM((npair, LANES), f32)] * 2
    half_gain = [pltpu.VMEM((half_pairs, LANES), f32)] * 2
    hbm = pl.BlockSpec(memory_space=pl.ANY)
    steps = n // 2
    staged = pl.pallas_call(
        functools.partial(fused_kernel, count, dims),
        out_shape=[jax.ShapeDtypeStruct(values.shape, bf16)] * 2,
        in_specs=[SM] * 2 + [VM] * 5 + [hbm] * 5,
        out_specs=[hbm] * 2,
        scratch_shapes=[
            pltpu.VMEM((tokens, hidden.shape[1]), bf16),
            pltpu.VMEM((n, 4, packed, gw), bf16), pltpu.VMEM((n, 4, wrows, gw), bf16),
            pltpu.VMEM((packed, gw), bf16), pltpu.VMEM((wrows, gw), bf16),
            pltpu.VMEM((tokens, width), bf16), pltpu.VMEM((tokens, width), bf16),
            *[pltpu.VMEM((tokens, gw), bf16)] * 4,
            pltpu.VMEM((tokens, 2 * gw + 2 * LANES), f32),
            pltpu.VMEM((tokens, heads), f32), pltpu.VMEM((tokens, heads), f32),
            pltpu.VMEM((1, heads), f32), pltpu.VMEM((1, heads), f32),
            *work, *work, *kept, *kept, *box * 9, *gain * 2, *half_gain * 2,
            dma((9,)), dma((2, steps, 2)), dma((2, steps, 4)), dma((n, 2)), dma((n, 2)),
            dma((2,)), dma((2,)), dma((2,)), dma((2,)), dma((4,)), dma((4,)),
            dma((2,)), dma((2, half_pairs)), dma((2,)), dma((2, half_pairs)),
            dma((2,)), dma((2, half_pairs // BATCH)), dma((2,)),
        ],
        compiler_params=pltpu.CompilerParams(
            collective_id=2, has_side_effects=True, vmem_limit_bytes=67_043_328),
        name="fused",
    )(seg_next, seg_prev, dt_bias[None], decay_rate[None], skip_gain[None], proj_dt, dt_prev.T,
      hidden, values, proj_bc, bc_prev, grad)
    chunk = pltpu.VMEM((tokens, width), bf16)
    return pl.pallas_call(
        hand_over,
        out_shape=[jax.ShapeDtypeStruct(values.shape, bf16)] * 2,
        in_specs=[hbm] * 2,
        out_specs=[hbm] * 2,
        scratch_shapes=[chunk, chunk, dma((2, HAND_PARTS)), dma((2,))],
        name="hand_over",
    )(*staged)


HAND_PARTS = 4


def hand_over(a_in, b_in, a_out, b_out, a_buf, b_buf, in_sem, out_sem):
    part = a_in.shape[0] // HAND_PARTS
    reads, writes = [], []
    for p in range(HAND_PARTS):
        rows = pl.ds(p * part, part)
        for k, (src, buf, dst) in enumerate(((a_in, a_buf, a_out), (b_in, b_buf, b_out))):
            reads.append(pltpu.make_async_copy(src.at[rows, :], buf.at[rows, :], in_sem.at[k, p]))
            writes.append(pltpu.make_async_copy(buf.at[rows, :], dst.at[rows, :], out_sem.at[k]))
    for copy in reads:
        copy.start()
    for read, write in zip(reads, writes):
        read.wait()
        write.start()
    for k, (buf, dst) in enumerate(((a_buf, a_out), (b_buf, b_out))):
        pltpu.make_async_copy(buf, dst, out_sem.at[k]).wait()


def body(
    hidden_next, values_next, seg_next, proj_bc, proj_dt, dt_bias, decay_rate, skip_gain,
    bc_prev, dt_prev, seg_prev, grad_prev,
):
    tokens_dev = hidden_next.shape[0]
    bc_width = proj_bc.shape[1]
    heads_all = proj_dt.shape[1]
    fsdp_count = lax.axis_size("fsdp")
    fsdp_place = lax.axis_index("fsdp")
    seq_count = lax.axis_size("seq")
    heads_dev = heads_all // fsdp_count
    state_dim = bc_width // (2 * GW)
    per_group = heads_all // GW
    groups_dev = max(1, heads_dev // per_group)
    first_head = fsdp_place * heads_dev
    first_group = first_head // per_group
    rows_dev = proj_bc.shape[0]
    half = bc_width // 2
    gw = groups_dev * state_dim

    if fsdp_count == 2 and seq_count % 4 == 0 and seq_count >= 8 and heads_all == LANES \
            and rows_dev == 2 * LANES and groups_dev * per_group == heads_dev:
        return fused(hidden_next, values_next, seg_next, proj_bc, proj_dt, dt_bias, decay_rate,
                     skip_gain, bc_prev, dt_prev, seg_prev, grad_prev, gw)

    blocks = []
    for f in range(fsdp_count):
        g0 = (f * heads_dev // per_group) * state_dim
        blocks.append([proj_bc[:, g0:g0 + gw], proj_bc[:, half + g0:half + g0 + gw]])
    ring = fsdp_count == 2 and seq_count % 4 == 0 and rows_dev % (2 * LANES) == 0 and heads_all == LANES
    if ring:
        shard = jnp.concatenate([*blocks[0], *blocks[1], proj_dt], axis=1)
        bc_next, dt_sum = gathered_sums(hidden_next, shard, 2 * gw)
        dt_sum = lax.dynamic_slice_in_dim(dt_sum, first_head, heads_dev, 1)
    else:
        pieces = []
        for f in range(fsdp_count):
            pieces += [*blocks[f], proj_dt[:, f * heads_dev:(f + 1) * heads_dev]]
        weights = lax.all_gather(jnp.concatenate(pieces, axis=1), "seq", axis=0, tiled=True)
        owned = lax.dynamic_slice_in_dim(
            hidden_next.reshape(tokens_dev, seq_count, fsdp_count, rows_dev), fsdp_place, 1, 2
        ).reshape(tokens_dev, seq_count * rows_dev)
        sums = lax.psum_scatter(jnp.dot(owned, weights, preferred_element_type=jnp.float32),
                                "fsdp", scatter_dimension=1, tiled=True)
        bc_next, dt_sum = sums[:, :2 * gw].astype(jnp.bfloat16), sums[:, 2 * gw:]

    decay = lax.dynamic_slice_in_dim(decay_rate, first_head, heads_dev, 0)[None]
    skip = lax.dynamic_slice_in_dim(skip_gain, first_head, heads_dev, 0)[None]
    bias = lax.dynamic_slice_in_dim(dt_bias, first_head, heads_dev, 0)[None]

    b_prev = lax.dynamic_slice_in_dim(bc_prev, first_group * state_dim, gw, 1)
    c_prev = lax.dynamic_slice_in_dim(bc_prev, half + first_group * state_dim, gw, 1)
    b_next, c_next = bc_next[:, :gw], bc_next[:, gw:]
    dt_next = jax.nn.softplus(dt_sum + bias)
    out_next, grad_values = chains(
        seg_next, values_next, c_next, b_next, dt_next, decay, skip,
        seg_prev, grad_prev, b_prev, c_prev, dt_prev)
    return (out_next, grad_values)


def solution(mesh):
    in_specs = (
        P("seq", None), P("seq", "fsdp"), P(), P(("seq", "fsdp"), None), P(("seq", "fsdp"), None),
        P(), P(), P(), P("seq", None), P("seq", "fsdp"), P(), P("seq", "fsdp"),
    )
    out_specs = (P("seq", "fsdp"), P("seq", "fsdp"))
    return jax.shard_map(body, mesh=mesh, in_specs=in_specs, out_specs=out_specs, check_vma=False)
```
